256 devices in a mesh: expert: 8 (over x, core), replica: 32 (over y, z).
Axes of the slice: x: 4, y: 4, z: 8, core: 2. Of those that a mesh axis runs over, the one named last changes fastest.
Arguments:
- tokens: bfloat16 [1536, 4096], P(('expert', 'replica')), may hold values from -6 to 6
- out_grad: bfloat16 [1536, 4096], P(('expert', 'replica')), may hold values from -2.5 to 2.5
- expert_ids: int32 [1536, 2], P(('expert', 'replica')), may hold values from 0 to 7, all different within a row; in each aligned block of 6 rows (0 to 5, 6 to 11, ...) at most 2 rows name the same one
- gates: float32 [1536, 2], P(('expert', 'replica')), may hold values from 0.1 to 1
- w_gate: bfloat16 [8, 7168, 4096], P('expert', 'replica'), may hold values from -0.09375 to 0.09375
- w_up: bfloat16 [8, 7168, 4096], P('expert', 'replica'), may hold values from -0.09375 to 0.09375
- w_down: bfloat16 [8, 7168, 4096], P('expert', 'replica'), may hold values from -0.0625 to 0.0625
Outputs:
- gate_grad: float32 [1536, 2], P(('expert', 'replica'))
- input_grad: bfloat16 [1536, 4096], P(('expert', 'replica'))
- grad_gate: bfloat16 [8, 7168, 4096], P('expert', 'replica')
- grad_up: bfloat16 [8, 7168, 4096], P('expert', 'replica')
- grad_down: bfloat16 [8, 7168, 4096], P('expert', 'replica')
The draws below stay inside these ranges and needn't reach their ends.
Inputs may be any that keep to these rules, and one draw needn't show every extreme that they name: `expert_ids`: each row names 2 different experts; among the rows of one device no expert is named more than 2 times.
All inputs are finite; a program needn't handle non-finite values.
Results may differ from the reference program's by a relative error of at most 0.02.
Values may be sent and summed in bfloat16 or wider, within the bound.
No kernel may reach another device: no remote copies, remote signals or barrier semaphores. Data moves between devices by JAX's collectives and lax.ppermute only.
A program may use at most 128 MiB of HBM per device.

```python
import math
import jax
import jax.numpy as jnp
import numpy as np
from jax import lax

D = 4096
FF = 7168
TOP = 2
TOK_DEV = 6
EXPERTS = 8
CAP = 2
TOKENS = 1536


def block_levels(key, dims, split, least, top_value):
    factor_of, own = 1.0, jax.random.fold_in(key, 6)
    for dim, shards_of in split:
        steps = jnp.exp(jax.random.uniform(jax.random.fold_in(own, dim), (shards_of,), jnp.float32, least / len(split), top_value / len(split)))
        factor_of = factor_of * jnp.repeat(steps, dims[dim] // shards_of).reshape([-1 if axis == dim else 1 for axis in range(len(dims))])
    return factor_of


def routed_block(stream_key, own, number, rows, count, top, bound, lean):
    ranking = jax.random.permutation(stream_key, count)
    crowded, usual = shares(count, rows * top, bound, lean, True), shares(count, rows * top, bound, lean, False)
    places = jnp.arange(count)

    def named(tallies, rotation):
        used = int((tallies > 0).sum())
        fixed = max(1, used // 4)
        passed = fixed + (places - fixed + rotation * (used - fixed)) % max(1, count - fixed)
        return jnp.zeros((count,), jnp.int32).at[ranking[jnp.where(places < fixed, places, passed)]].set(jnp.asarray(tallies, jnp.int32))

    tallies = jnp.where(number % 4 == 0, named(crowded, number // 4), named(usual, number - number // 4 - 1))
    mixed = jax.random.permutation(jax.random.fold_in(own, 3), count)
    source_of, sink = mixed[0:count // 2 * 2:2], mixed[1:count // 2 * 2:2]
    margin = jnp.minimum(tallies[source_of] - 1, bound - tallies[sink]) // 2
    margin = jnp.where((source_of == ranking[0]) | (sink == ranking[0]) | (tallies[sink] == 0), 0, jnp.maximum(margin, 0))
    passed = jax.random.randint(jax.random.fold_in(own, 4), (count // 2,), 0, 1 << 20) % (margin + 1)
    tallies = tallies.at[source_of].add(-passed).at[sink].add(passed)
    labels = jnp.searchsorted(jnp.cumsum(tallies), jnp.arange(rows * top), side="right").astype(jnp.int32)
    listing = labels.reshape(top, rows).T
    listing = listing[jax.random.permutation(jax.random.fold_in(own, 1), rows)]
    rotation = jax.random.randint(jax.random.fold_in(own, 2), (rows, 1), 0, top)
    return jnp.take_along_axis(listing, (jnp.arange(top)[None, :] + rotation) % top, axis=1)


def shares(amount, total, reach, skew, full):
    weights = [(1 << 20) // math.isqrt(grade ** skew) + 1 for grade in range(1, amount + 1)]
    largest = reach if full else min(reach, max(-(-total // amount), total * weights[0] // sum(weights)))
    least = 1 if total - largest >= amount - 1 else 0
    holding, spare = [largest] + [least] * (amount - 1), total - largest - least * (amount - 1)
    while spare > 0:
        candidates = [i for i in range(1, amount) if holding[i] < largest] or [i for i in range(1, amount) if holding[i] < reach]
        whole, left = sum([weights[i] for i in candidates]), spare
        for i in candidates:
            extra = min(reach - holding[i], max(1, left * weights[i] // whole), spare)
            holding[i] = holding[i] + extra
            spare = spare - extra
    return np.array(holding)


def bell_draw(rng, shape, scale, limit, shards=(), kind=jnp.bfloat16):
    drawn = scale * jax.random.normal(rng, shape, jnp.float32)
    if shards:
        drawn = drawn * block_levels(rng, shape, shards, -0.22, 0.18)
    return jnp.clip(drawn, -limit, limit).astype(kind)


def setup_inputs(seed: int = 0) -> dict:
    streams_of = jax.random.split(jax.random.key(seed), 8)
    tokens = bell_draw(streams_of[0], (TOKENS, D), 1.0, 6.0, ((0, 256),))
    out_grad = bell_draw(streams_of[1], (TOKENS, D), 0.3, 2.5, ((0, 256),))
    expert_ids_keys = jax.random.split(jax.random.fold_in(streams_of[2], 1), TOKENS // TOK_DEV)
    expert_ids_turns = jax.random.permutation(jax.random.fold_in(streams_of[2], 3), TOKENS // TOK_DEV)
    expert_ids = jax.vmap(lambda own, number: routed_block(jax.random.fold_in(streams_of[2], 2), own, number, TOK_DEV, EXPERTS, TOP, CAP, 2))(expert_ids_keys, expert_ids_turns).reshape((TOKENS, TOP))
    gates = jnp.clip(0.1 + 0.9 * jax.random.uniform(streams_of[3], (TOKENS, TOP), jnp.float32) ** block_levels(streams_of[3], (TOKENS, TOP), ((0, 256),), -0.2, 0.2), 0.1, 1.0)
    w_gate = bell_draw(streams_of[4], (EXPERTS, FF, D), D ** -0.5, 0.09375, ((0, 8), (1, 32)))
    w_up = bell_draw(streams_of[5], (EXPERTS, FF, D), D ** -0.5, 0.09375, ((0, 8), (1, 32)))
    w_down = bell_draw(streams_of[6], (EXPERTS, FF, D), FF ** -0.5, 0.0625, ((0, 8), (1, 32)))
    return {"tokens": tokens, "out_grad": out_grad, "expert_ids": expert_ids, "gates": gates, "w_gate": w_gate, "w_up": w_up, "w_down": w_down}


def reference(tokens, out_grad, expert_ids, gates, w_gate, w_up, w_down):
    token_count = tokens.shape[0]
    model_width = tokens.shape[1]
    blocks = token_count // TOK_DEV
    per_block = TOK_DEV * TOP
    block_ids = expert_ids.reshape(blocks, per_block)
    sequence_pos = jnp.arange(per_block, dtype=jnp.int32)
    earlier = sequence_pos[None, :] < sequence_pos[:, None]
    same_expert = block_ids[:, :, None] == block_ids[:, None, :]
    slot_rank = jnp.sum(jnp.logical_and(same_expert, earlier[None, :, :]), axis=2).astype(jnp.int32)
    position = (jnp.arange(blocks, dtype=jnp.int32)[:, None] * CAP + slot_rank).reshape(-1)
    expert_flat = block_ids.reshape(-1).astype(jnp.int32)
    token_flat = jnp.repeat(jnp.arange(token_count, dtype=jnp.int32), TOP)
    slot_total = blocks * CAP
    source = jnp.full((EXPERTS, slot_total), token_count, jnp.int32).at[expert_flat, position].set(token_flat)
    slot_gate = jnp.zeros((EXPERTS, slot_total), jnp.float32).at[expert_flat, position].set(gates.reshape(-1).astype(jnp.float32))
    padded_tokens = jnp.concatenate([tokens, jnp.zeros((1, model_width), tokens.dtype)], axis=0)
    padded_grad = jnp.concatenate([out_grad, jnp.zeros((1, model_width), out_grad.dtype)], axis=0)
    contract = (((1,), (1,)), ((), ()))
    leading = (((0,), (0,)), ((), ()))

    def one_expert(expert_index):
        gathered = padded_tokens[source[expert_index]]
        gathered_grad = padded_grad[source[expert_index]]
        gate_weight = w_gate[expert_index]
        up_weight = w_up[expert_index]
        down_weight = w_down[expert_index]
        gate_pre = lax.dot_general(gathered, gate_weight, contract, preferred_element_type=jnp.float32)
        up_pre = lax.dot_general(gathered, up_weight, contract, preferred_element_type=jnp.float32)
        sigmoid_gate = jax.nn.sigmoid(gate_pre)
        active = gate_pre * sigmoid_gate
        hidden = (active * up_pre).astype(jnp.bfloat16)
        expert_out = jnp.dot(hidden, down_weight, preferred_element_type=jnp.float32)
        products = jnp.sum(gathered_grad.astype(jnp.float32) * expert_out, axis=1)
        scaled = (slot_gate[expert_index][:, None] * gathered_grad.astype(jnp.float32)).astype(jnp.bfloat16)
        hidden_grad = lax.dot_general(scaled, down_weight, contract, preferred_element_type=jnp.float32)
        gate_pre_grad = (hidden_grad * up_pre * sigmoid_gate * (1.0 + gate_pre * (1.0 - sigmoid_gate))).astype(jnp.bfloat16)
        up_pre_grad = (hidden_grad * active).astype(jnp.bfloat16)
        grad_down = lax.dot_general(hidden, scaled, leading, preferred_element_type=jnp.float32).astype(jnp.bfloat16)
        grad_gate = lax.dot_general(gate_pre_grad, gathered, leading, preferred_element_type=jnp.float32).astype(jnp.bfloat16)
        grad_up = lax.dot_general(up_pre_grad, gathered, leading, preferred_element_type=jnp.float32).astype(jnp.bfloat16)
        slot_grad = (jnp.dot(gate_pre_grad, gate_weight, preferred_element_type=jnp.float32) + jnp.dot(up_pre_grad, up_weight, preferred_element_type=jnp.float32)).astype(jnp.bfloat16)
        return products, slot_grad, grad_gate, grad_up, grad_down

    products, slot_grad, grad_gate, grad_up, grad_down = lax.map(one_expert, jnp.arange(EXPERTS, dtype=jnp.int32))
    gate_grad = products[expert_flat, position].reshape(token_count, TOP)
    picked = slot_grad[expert_flat, position].astype(jnp.float32).reshape(token_count, TOP, model_width)
    input_grad = jnp.sum(picked, axis=1).astype(jnp.bfloat16)
    return gate_grad, input_grad, grad_gate, grad_up, grad_down
```

```python
import jax
import jax.numpy as jnp
from jax import lax
from jax.sharding import Mesh
from jax.sharding import PartitionSpec as P

REPLICA = ("replica_0", "replica_1")
EXPERT_REPLICA = ("expert", "replica_0", "replica_1")
HOME = ("replica_0", "expert")


def on_device(tokens, out_grad, expert_ids, gates, w_gate, w_up, w_down):
    token_count = tokens.shape[0]
    fan_out = expert_ids.shape[1]
    model_width = tokens.shape[1]
    owners = lax.axis_size("expert")
    rows_y = lax.axis_size("replica_0")
    rows_z = lax.axis_size("replica_1")
    capacity = max(2, 4 * token_count * fan_out // (3 * owners))
    slot_count = owners * capacity
    flat_ids = expert_ids.reshape(-1)
    sequence_pos = jnp.arange(token_count * fan_out, dtype=jnp.int32)
    earlier = sequence_pos[None, :] < sequence_pos[:, None]
    same_expert = flat_ids[:, None] == flat_ids[None, :]
    slot_rank = jnp.sum(jnp.logical_and(same_expert, earlier), axis=1)
    target = flat_ids * capacity + slot_rank
    token_hot = (target[:, None] == jnp.arange(slot_count, dtype=jnp.int32)[None, :]).astype(
        jnp.float32
    )
    token_hot = token_hot.reshape(token_count, fan_out, slot_count)
    dispatch = jnp.sum(token_hot, axis=1).astype(jnp.bfloat16)
    slot_gate = jnp.sum(token_hot * gates[:, :, None], axis=(0, 1))
    leading = (((0,), (0,)), ((), ()))
    contract = (((1,), (1,)), ((), ()))
    picked = lax.dot_general(
        dispatch,
        jnp.concatenate([tokens, out_grad], axis=1),
        leading,
        preferred_element_type=jnp.float32,
    )
    scale = jnp.concatenate(
        [
            jnp.ones((slot_count, model_width), jnp.float32),
            jnp.broadcast_to(slot_gate[:, None], (slot_count, model_width)),
        ],
        axis=1,
    )
    send = (picked * scale).astype(jnp.bfloat16)
    gate_weight = w_gate[0]
    up_weight = w_up[0]
    down_weight = w_down[0]
    owned = lax.all_to_all(
        send.reshape(owners, capacity, 2 * model_width), "expert", 0, 0, tiled=True
    ).reshape(slot_count, 2 * model_width)
    column = lax.all_gather(owned, REPLICA, axis=0, tiled=True)
    gathered = column[:, :model_width]
    scaled = column[:, model_width:]
    gate_pre = lax.dot_general(gathered, gate_weight, contract, preferred_element_type=jnp.float32)
    up_pre = lax.dot_general(gathered, up_weight, contract, preferred_element_type=jnp.float32)
    hidden_grad = lax.dot_general(scaled, down_weight, contract, preferred_element_type=jnp.float32)
    sigmoid_gate = jax.nn.sigmoid(gate_pre)
    active = gate_pre * sigmoid_gate
    hidden = (active * up_pre).astype(jnp.bfloat16)
    partial_value = jnp.sum(hidden.astype(jnp.float32) * hidden_grad, axis=1)
    gate_pre_grad = (
        hidden_grad * up_pre * sigmoid_gate * (1.0 + gate_pre * (1.0 - sigmoid_gate))
    ).astype(jnp.bfloat16)
    up_pre_grad = (hidden_grad * active).astype(jnp.bfloat16)

    def by_z(value):
        tiles = value.reshape(rows_y, rows_z, slot_count, value.shape[1])
        return jnp.swapaxes(tiles, 0, 1).reshape(value.shape)

    slot_grad = (
        jnp.dot(by_z(gate_pre_grad), gate_weight, preferred_element_type=jnp.float32)
        + jnp.dot(by_z(up_pre_grad), up_weight, preferred_element_type=jnp.float32)
    ).astype(jnp.bfloat16)
    summed_z = lax.psum_scatter(slot_grad, "replica_1", scatter_dimension=0, tiled=True)
    tiles = lax.all_to_all(
        partial_value.reshape(rows_y * rows_z, slot_count), REPLICA, 0, 0, tiled=True
    )
    returned = lax.all_to_all(
        jnp.sum(tiles, axis=0).reshape(owners, capacity), "expert", 0, 0, tiled=True
    )
    product = jnp.sum(token_hot * returned.reshape(-1)[None, None, :], axis=2)
    gate_grad = product / gates
    grad_down = lax.dot_general(hidden, scaled, leading, preferred_element_type=jnp.float32).astype(
        jnp.bfloat16
    )
    grad_gate = lax.dot_general(
        gate_pre_grad, gathered, leading, preferred_element_type=jnp.float32
    ).astype(jnp.bfloat16)
    grad_up = lax.dot_general(
        up_pre_grad, gathered, leading, preferred_element_type=jnp.float32
    ).astype(jnp.bfloat16)
    slot_back = lax.all_to_all(
        summed_z.reshape(rows_y * owners, capacity, model_width), HOME, 0, 0, tiled=True
    ).reshape(rows_y * slot_count, model_width)
    input_grad = jnp.dot(
        jnp.concatenate([dispatch] * rows_y, axis=1),
        slot_back,
        preferred_element_type=jnp.float32,
    ).astype(jnp.bfloat16)
    return (gate_grad, input_grad, grad_gate[None], grad_up[None], grad_down[None])


def solution(mesh):
    torus = Mesh(
        mesh.devices.reshape(mesh.shape["expert"], 4, 8), ("expert", "replica_0", "replica_1")
    )
    in_specs = (
        P(EXPERT_REPLICA, None),
        P(EXPERT_REPLICA, None),
        P(EXPERT_REPLICA, None),
        P(EXPERT_REPLICA, None),
        P("expert", REPLICA, None),
        P("expert", REPLICA, None),
        P("expert", REPLICA, None),
    )
    out_specs = (
        P(EXPERT_REPLICA, None),
        P(EXPERT_REPLICA, None),
        P("expert", REPLICA, None),
        P("expert", REPLICA, None),
        P("expert", REPLICA, None),
    )
    return jax.shard_map(
        on_device, mesh=torus, in_specs=in_specs, out_specs=out_specs, check_vma=False
    )
```

```python
import jax
import jax.numpy as jnp
from jax import lax
from jax.sharding import Mesh
from jax.sharding import PartitionSpec as P

REPLICA = ("replica_0", "replica_1")
EXPERT_REPLICA = ("expert", "replica_0", "replica_1")
Y = "replica_0"
Z = "replica_1"
LANES = 128
SPLIT = 2560


def pass_on(value, axis, back):
    peers = lax.axis_size(axis)
    return lax.ppermute(value, axis, [((i + back) % peers, i) for i in range(peers)])


def stack(blocks):
    return jnp.concatenate(blocks, axis=0)


def direct(value, axis):
    return [value] + [pass_on(value, axis, k) for k in range(1, lax.axis_size(axis))]


def ring(value, axis):
    middle = lax.axis_size(axis) // 2
    half = value.shape[0] // 2
    ahead = [pass_on(value, axis, 1)]
    behind = [pass_on(value, axis, -1)]
    for _ in range(middle - 2):
        ahead.append(pass_on(ahead[-1], axis, 1))
        behind.append(pass_on(behind[-1], axis, -1))
    first = pass_on(ahead[-1][:half], axis, 1)
    last = pass_on(behind[-1][half:], axis, -1)
    return [value] + ahead + [stack([first, last])] + behind[::-1]


def far_first(peers):
    return sorted(range(1, peers), key=lambda k: -min(k, peers - k))


def halves(value):
    high = lax.reduce_precision(value, 8, 7)
    low = (value - high).astype(jnp.bfloat16)
    high = high.astype(jnp.bfloat16)
    lane = lax.broadcasted_iota(jnp.int32, (*value.shape, LANES), value.ndim)
    zero = jnp.zeros((), jnp.bfloat16)
    return jnp.where(lane == 0, high[..., None], jnp.where(lane == 1, low[..., None], zero))


def joined(columns):
    return columns[..., 0].astype(jnp.float32) + columns[..., 1].astype(jnp.float32)


def own_sum(own, own_columns, arrived):
    wide = own.shape[-1]
    total = own.astype(jnp.float32)
    value = joined(own_columns)
    for block in arrived:
        total = total + block[..., :wide]
        value = value + joined(block[..., wide:])
    return total, value


def on_device(tokens, out_grad, expert_ids, gates, w_gate, w_up, w_down):
    token_count = tokens.shape[0]
    fan_out = expert_ids.shape[1]
    model_width = tokens.shape[1]
    owners = lax.axis_size("expert")
    rows_y = lax.axis_size("replica_0")
    rows_z = lax.axis_size("replica_1")
    capacity = max(2, 4 * token_count * fan_out // (3 * owners))
    slot_count = owners * capacity
    flat_ids = expert_ids.reshape(-1)
    sequence_pos = jnp.arange(token_count * fan_out, dtype=jnp.int32)
    earlier = sequence_pos[None, :] < sequence_pos[:, None]
    same_expert = flat_ids[:, None] == flat_ids[None, :]
    slot_rank = jnp.sum(jnp.logical_and(same_expert, earlier), axis=1)
    target = flat_ids * capacity + slot_rank
    token_hot = (target[:, None] == jnp.arange(slot_count, dtype=jnp.int32)[None, :]).astype(
        jnp.float32
    )
    token_hot = token_hot.reshape(token_count, fan_out, slot_count)
    dispatch = jnp.sum(token_hot, axis=1).astype(jnp.bfloat16)
    slot_gate = jnp.sum(token_hot * gates[:, :, None], axis=(0, 1))
    leading = (((0,), (0,)), ((), ()))
    contract = (((1,), (1,)), ((), ()))
    picked = lax.dot_general(
        dispatch,
        jnp.concatenate([tokens, out_grad], axis=1),
        leading,
        preferred_element_type=jnp.float32,
    )
    scale = jnp.concatenate(
        [
            jnp.ones((slot_count, model_width), jnp.float32),
            jnp.broadcast_to(slot_gate[:, None], (slot_count, model_width)),
        ],
        axis=1,
    )
    send = (picked * scale).astype(jnp.bfloat16)
    gate_weight = w_gate[0]
    up_weight = w_up[0]
    down_weight = w_down[0]
    owned = lax.all_to_all(
        send.reshape(owners, capacity, 2 * model_width), "expert", 0, 0, tiled=True
    ).reshape(slot_count, 2 * model_width)
    scaled_y = stack(direct(owned[:, model_width:], Y))
    tokens_z = stack(ring(owned[:, :model_width], Z))
    token_blocks = ring(tokens_z, Y)
    scaled_blocks = ring(scaled_y, Z)

    def forward(blocks, weight):
        return stack(
            [
                lax.dot_general(block, weight, contract, preferred_element_type=jnp.float32)
                for block in blocks
            ]
        )

    def flip(value, outer):
        tiles = value.reshape(outer, -1, slot_count, value.shape[1])
        return jnp.swapaxes(tiles, 0, 1).reshape(value.shape)

    gate_pre = forward(token_blocks, gate_weight)
    up_pre = forward(token_blocks, up_weight)
    hidden_grad = flip(forward(scaled_blocks, down_weight), rows_z)
    sigmoid_gate = jax.nn.sigmoid(gate_pre)
    active = gate_pre * sigmoid_gate
    hidden = (active * up_pre).astype(jnp.bfloat16)
    partial_value = jnp.sum(hidden.astype(jnp.float32) * hidden_grad, axis=1)
    gate_pre_grad = (
        hidden_grad * up_pre * sigmoid_gate * (1.0 + gate_pre * (1.0 - sigmoid_gate))
    ).astype(jnp.bfloat16)
    up_pre_grad = (hidden_grad * active).astype(jnp.bfloat16)

    def slot_part(gate_side, up_side, first, last):
        return (
            jnp.dot(gate_side, gate_weight[:, first:last], preferred_element_type=jnp.float32)
            + jnp.dot(up_side, up_weight[:, first:last], preferred_element_type=jnp.float32)
        ).astype(jnp.bfloat16)

    part_a = slot_part(gate_pre_grad, up_pre_grad, 0, SPLIT)
    part_b = slot_part(flip(gate_pre_grad, rows_y), flip(up_pre_grad, rows_y), SPLIT, model_width)
    tiles_a = part_a.reshape(rows_y, rows_z * slot_count, SPLIT)
    tiles_b = part_b.reshape(rows_z, rows_y * slot_count, model_width - SPLIT)
    tiles_v = halves(partial_value.reshape(rows_y, rows_z * slot_count))
    sum_a, sum_v = own_sum(
        tiles_a[0],
        tiles_v[0],
        [
            pass_on(jnp.concatenate([tiles_a[k], tiles_v[k]], axis=1), Y, -k)
            for k in range(1, rows_y)
        ],
    )
    sum_b = jnp.float32(0) + tiles_b[0]
    for k in far_first(rows_z):
        sum_b = sum_b + pass_on(tiles_b[k], Z, -k)
    tiles_a = sum_a.astype(jnp.bfloat16).reshape(rows_z, slot_count, SPLIT)
    tiles_v = halves(sum_v.reshape(rows_z, slot_count))
    tiles_b = sum_b.astype(jnp.bfloat16).reshape(rows_y, slot_count, model_width - SPLIT)
    sum_a, sum_v = own_sum(
        tiles_a[0],
        tiles_v[0],
        [
            pass_on(jnp.concatenate([tiles_a[k], tiles_v[k]], axis=1), Z, -k)
            for k in far_first(rows_z)
        ],
    )
    sum_b = jnp.float32(0) + tiles_b[0]
    for k in range(1, rows_y):
        sum_b = sum_b + pass_on(tiles_b[k], Y, -k)
    slot_home = jnp.concatenate(
        [sum_a.astype(jnp.bfloat16), sum_b.astype(jnp.bfloat16), halves(sum_v)], axis=1
    )
    gathered = stack(token_blocks)
    scaled = stack(scaled_blocks)
    grad_down = lax.dot_general(
        flip(hidden, rows_y), scaled, leading, preferred_element_type=jnp.float32
    ).astype(jnp.bfloat16)
    grad_gate = lax.dot_general(
        gate_pre_grad, gathered, leading, preferred_element_type=jnp.float32
    ).astype(jnp.bfloat16)
    grad_up = lax.dot_general(
        up_pre_grad, gathered, leading, preferred_element_type=jnp.float32
    ).astype(jnp.bfloat16)
    slot_back = lax.all_to_all(
        slot_home.reshape(owners, capacity, model_width + LANES), "expert", 0, 0, tiled=True
    ).reshape(slot_count, model_width + LANES)
    input_grad = jnp.dot(
        dispatch, slot_back[:, :model_width], preferred_element_type=jnp.float32
    ).astype(jnp.bfloat16)
    returned = joined(slot_back[:, model_width:])
    product = jnp.sum(token_hot * returned[None, None, :], axis=2)
    gate_grad = product / gates
    return (gate_grad, input_grad, grad_gate[None], grad_up[None], grad_down[None])


def solution(mesh):
    torus = Mesh(
        mesh.devices.reshape(mesh.shape["expert"], 4, 8), ("expert", "replica_0", "replica_1")
    )
    in_specs = (
        P(EXPERT_REPLICA, None),
        P(EXPERT_REPLICA, None),
        P(EXPERT_REPLICA, None),
        P(EXPERT_REPLICA, None),
        P("expert", REPLICA, None),
        P("expert", REPLICA, None),
        P("expert", REPLICA, None),
    )
    out_specs = (
        P(EXPERT_REPLICA, None),
        P(EXPERT_REPLICA, None),
        P("expert", REPLICA, None),
        P("expert", REPLICA, None),
        P("expert", REPLICA, None),
    )
    return jax.shard_map(
        on_device, mesh=torus, in_specs=in_specs, out_specs=out_specs, check_vma=False
    )
```

```python
import functools

import jax
import jax.numpy as jnp
from jax import lax
from jax.experimental import pallas as pl
from jax.experimental.pallas import tpu as pltpu
from jax.sharding import Mesh
from jax.sharding import PartitionSpec as P


REPLICA = ("replica_0", "replica_1")
EXPERT_REPLICA = ("expert", "replica_0", "replica_1")
Y = "replica_0"
Z = "replica_1"
LANES = 128
SPLIT = 2560
CHUNK = 512
VMEM = pl.BlockSpec(memory_space=pltpu.VMEM)
LIMIT = pltpu.CompilerParams(vmem_limit_bytes=16 * 1024 * 1024)
SMALL = pltpu.CompilerParams(vmem_limit_bytes=8 * 1024 * 1024)
CONTRACT = (((1,), (1,)), ((), ()))
LEADING = (((0,), (0,)), ((), ()))


def pass_on(value, axis, back):
    peers = lax.axis_size(axis)
    return lax.ppermute(value, axis, [((i + back) % peers, i) for i in range(peers)])


def direct(value, axis):
    return [value] + [pass_on(value, axis, k) for k in range(1, lax.axis_size(axis))]


def ring(value, axis):
    middle = lax.axis_size(axis) // 2
    half = value.shape[0] // 2
    ahead = [pass_on(value, axis, 1)]
    behind = [pass_on(value, axis, -1)]
    for _ in range(middle - 2):
        ahead.append(pass_on(ahead[-1], axis, 1))
        behind.append(pass_on(behind[-1], axis, -1))
    first = pass_on(ahead[-1][:half], axis, 1)
    last = pass_on(behind[-1][half:], axis, -1)
    return [value] + ahead + [first, last] + behind[::-1]


def far_first(peers):
    return sorted(range(1, peers), key=lambda k: -min(k, peers - k))


def high_low(value):
    high = value.astype(jnp.bfloat16)
    low = (value - high.astype(jnp.float32)).astype(jnp.bfloat16)
    lane = lax.broadcasted_iota(jnp.int32, (value.shape[0], LANES), 1)
    both = jnp.where(
        lane == 0,
        high.astype(jnp.float32),
        jnp.where(lane == 1, low.astype(jnp.float32), jnp.float32(0)),
    )
    return both.astype(jnp.bfloat16)


def joined(columns):
    return jnp.sum(columns.astype(jnp.float32), axis=1, keepdims=True)


def main_kernel(rows_y, rows_z, slots, count_t, count_s, *refs):
    token_refs, refs = refs[:count_t], refs[count_t:]
    scaled_refs, refs = refs[:count_s], refs[count_s:]
    wg, wu, wd, t_all, s_all, hid_s, gpg_t, upg_t = refs[:8]
    refs = refs[8:]
    out_a, refs = refs[:rows_y], refs[rows_y:]
    out_b, refs = refs[:rows_z], refs[rows_z:]
    acc_g, acc_u, acc_h, val_s, gpg_s, upg_s = refs
    width = t_all.shape[1]
    total = rows_y * rows_z * slots
    acc_g[...] = jnp.zeros_like(acc_g)
    acc_u[...] = jnp.zeros_like(acc_u)
    acc_h[...] = jnp.zeros_like(acc_h)

    def forward(step, carry):
        cols = pl.ds(pl.multiple_of(step * CHUNK, CHUNK), CHUNK)
        for blocks, whole in ((token_refs, t_all), (scaled_refs, s_all)):
            row = 0
            for block in blocks:
                whole[row : row + block.shape[0], cols] = block[:, cols]
                row += block.shape[0]
        rows_t = t_all[:, cols]
        acc_g[...] += lax.dot_general(
            rows_t, wg[:, cols], CONTRACT, preferred_element_type=jnp.float32
        )
        acc_u[...] += lax.dot_general(
            rows_t, wu[:, cols], CONTRACT, preferred_element_type=jnp.float32
        )
        acc_h[...] += lax.dot_general(
            s_all[:, cols], wd[:, cols], CONTRACT, preferred_element_type=jnp.float32
        )
        return carry

    lax.fori_loop(0, width // CHUNK, forward, 0)

    for dy in range(rows_y):
        for dz in range(rows_z):
            at_t = (dy * rows_z + dz) * slots
            at_s = (dz * rows_y + dy) * slots
            here = slice(at_t, at_t + slots)
            there = slice(at_s, at_s + slots)
            gate_pre = acc_g[here, :]
            up_pre = acc_u[here, :]
            hidden_grad = acc_h[there, :]
            sigmoid_gate = jax.nn.sigmoid(gate_pre)
            active = gate_pre * sigmoid_gate
            hidden = (active * up_pre).astype(jnp.bfloat16)
            val_s[here, :] = high_low(
                jnp.sum(hidden.astype(jnp.float32) * hidden_grad, axis=1, keepdims=True)
            )
            gate_grad = (
                hidden_grad * up_pre * sigmoid_gate * (1.0 + gate_pre * (1.0 - sigmoid_gate))
            ).astype(jnp.bfloat16)
            up_grad = (hidden_grad * active).astype(jnp.bfloat16)
            hid_s[there, :] = hidden
            gpg_t[here, :] = gate_grad
            upg_t[here, :] = up_grad
            gpg_s[there, :] = gate_grad
            upg_s[there, :] = up_grad

    def slots_of(left, right, outs, shift):
        rows = total // len(outs)

        def step_of(step, carry):
            cols = pl.ds(pl.multiple_of(step * CHUNK, CHUNK), CHUNK)
            wide = pl.ds(pl.multiple_of(step * CHUNK + shift, CHUNK), CHUNK)
            value = (
                jnp.dot(left[...], wg[:, wide], preferred_element_type=jnp.float32)
                + jnp.dot(right[...], wu[:, wide], preferred_element_type=jnp.float32)
            ).astype(jnp.bfloat16)
            for k, out in enumerate(outs):
                out[:, cols] = value[k * rows : (k + 1) * rows]
            return carry

        return step_of

    lax.fori_loop(0, SPLIT // CHUNK, slots_of(gpg_t, upg_t, out_a, 0), 0)
    for k, out in enumerate(out_a):
        rows = total // rows_y
        out[:, SPLIT:] = val_s[k * rows : (k + 1) * rows, :]
    lax.fori_loop(0, (width - SPLIT) // CHUNK, slots_of(gpg_s, upg_s, out_b, SPLIT), 0)


def main_call(token_blocks, scaled_blocks, wg, wu, wd, rows_y, rows_z, slots):
    total = rows_y * rows_z * slots
    hidden, width = wg.shape
    bf = jnp.bfloat16
    shapes = [jax.ShapeDtypeStruct((total, width), bf)] * 2
    shapes += [jax.ShapeDtypeStruct((total, hidden), bf)] * 3
    shapes += [jax.ShapeDtypeStruct((total // rows_y, SPLIT + LANES), bf)] * rows_y
    shapes += [jax.ShapeDtypeStruct((total // rows_z, width - SPLIT), bf)] * rows_z
    blocks = list(token_blocks) + list(scaled_blocks)
    outs = pl.pallas_call(
        functools.partial(
            main_kernel, rows_y, rows_z, slots, len(token_blocks), len(scaled_blocks)
        ),
        out_shape=shapes,
        in_specs=[VMEM] * (len(blocks) + 3),
        out_specs=[VMEM] * len(shapes),
        scratch_shapes=[pltpu.VMEM((total, hidden), jnp.float32)] * 3
        + [pltpu.VMEM((total, LANES), bf)]
        + [pltpu.VMEM((total, hidden), bf)] * 2,
        compiler_params=LIMIT,
        cost_estimate=pl.CostEstimate(
            flops=10 * total * hidden * width, bytes_accessed=30 << 20, transcendentals=0
        ),
        name="experts",
    )(*blocks, wg, wu, wd)
    return outs[:5], outs[5 : 5 + rows_y], outs[5 + rows_y :]


def sum_a_kernel(slots, *refs):
    outs = refs[-(refs[0].shape[0] // slots) :]
    ins = refs[: len(refs) - len(outs)]
    for k, out in enumerate(outs):
        rows = slice(k * slots, (k + 1) * slots)
        total = ins[0][rows, :SPLIT].astype(jnp.float32)
        value = joined(ins[0][rows, SPLIT:])
        for ref in ins[1:]:
            total = total + ref[rows, :SPLIT].astype(jnp.float32)
            value = value + joined(ref[rows, SPLIT:])
        out[:, :SPLIT] = total.astype(jnp.bfloat16)
        out[:, SPLIT:] = high_low(value)


def sum_b_kernel(slots, *refs):
    count = len(refs)
    outs = refs[-(refs[0].shape[0] // slots) :]
    ins = refs[: count - len(outs)]
    for k, out in enumerate(outs):
        rows = slice(k * slots, (k + 1) * slots)
        total = ins[0][rows, :].astype(jnp.float32)
        for ref in ins[1:]:
            total = total + ref[rows, :].astype(jnp.float32)
        out[...] = total.astype(jnp.bfloat16)


def last_kernel(count, *refs):
    first, other_refs, out = refs[:count], refs[count:-1], refs[-1]
    total = first[0][:, :SPLIT].astype(jnp.float32)
    value = joined(first[0][:, SPLIT:])
    for ref in first[1:]:
        total = total + ref[:, :SPLIT].astype(jnp.float32)
        value = value + joined(ref[:, SPLIT:])
    other = other_refs[0][...].astype(jnp.float32)
    for ref in other_refs[1:]:
        other = other + ref[...].astype(jnp.float32)
    width = SPLIT + other.shape[1]
    out[:, :SPLIT] = total.astype(jnp.bfloat16)
    out[:, SPLIT:width] = other.astype(jnp.bfloat16)
    out[:, width:] = high_low(value)


def cost(count):
    return pl.CostEstimate(flops=count, bytes_accessed=3 * count, transcendentals=0)


def on_device(tokens, out_grad, expert_ids, gates, w_gate, w_up, w_down):
    token_count = tokens.shape[0]
    fan_out = expert_ids.shape[1]
    model_width = tokens.shape[1]
    owners = lax.axis_size("expert")
    rows_y = lax.axis_size(Y)
    rows_z = lax.axis_size(Z)
    capacity = max(2, 4 * token_count * fan_out // (3 * owners))
    slots = owners * capacity
    bf = jnp.bfloat16
    flat_ids = expert_ids.reshape(-1)
    sequence_pos = jnp.arange(token_count * fan_out, dtype=jnp.int32)
    earlier = sequence_pos[None, :] < sequence_pos[:, None]
    same_expert = flat_ids[:, None] == flat_ids[None, :]
    slot_rank = jnp.sum(jnp.logical_and(same_expert, earlier), axis=1)
    target = flat_ids * capacity + slot_rank
    token_hot = (target[:, None] == jnp.arange(slots, dtype=jnp.int32)[None, :]).astype(jnp.float32)
    token_hot = token_hot.reshape(token_count, fan_out, slots)
    dispatch = jnp.sum(token_hot, axis=1).astype(bf)
    slot_gate = jnp.sum(token_hot * gates[:, :, None], axis=(0, 1))
    picked = lax.dot_general(
        dispatch,
        jnp.concatenate([tokens, out_grad], axis=1),
        LEADING,
        preferred_element_type=jnp.float32,
    )
    scale = jnp.concatenate(
        [
            jnp.ones((slots, model_width), jnp.float32),
            jnp.broadcast_to(slot_gate[:, None], (slots, model_width)),
        ],
        axis=1,
    )
    send = (picked * scale).astype(bf)
    owned = lax.all_to_all(
        send.reshape(owners, capacity, 2 * model_width), "expert", 0, 0, tiled=True
    ).reshape(slots, 2 * model_width)
    scaled_y = jnp.concatenate(direct(owned[:, model_width:], Y), axis=0)
    tokens_z = jnp.concatenate(ring(owned[:, :model_width], Z), axis=0)
    token_blocks = ring(tokens_z, Y)
    scaled_blocks = ring(scaled_y, Z)
    (gathered, scaled, hidden, gate_pre_grad, up_pre_grad), out_a, out_b = main_call(
        token_blocks, scaled_blocks, w_gate[0], w_up[0], w_down[0], rows_y, rows_z, slots
    )
    arrived_b = [pass_on(out_b[k], Z, -k) for k in far_first(rows_z)]
    arrived_a = [pass_on(out_a[k], Y, -k) for k in range(1, rows_y)]
    wide = SPLIT + LANES
    tiles_a = pl.pallas_call(
        functools.partial(sum_a_kernel, slots),
        out_shape=[jax.ShapeDtypeStruct((slots, wide), bf)] * rows_z,
        in_specs=[VMEM] * rows_y,
        out_specs=[VMEM] * rows_z,
        compiler_params=SMALL,
        cost_estimate=cost(rows_y * rows_z * slots * wide),
        name="sum_y",
    )(out_a[0], *arrived_a)
    moved_a = [pass_on(tiles_a[k], Z, -k) for k in far_first(rows_z)]
    tiles_b = pl.pallas_call(
        functools.partial(sum_b_kernel, slots),
        out_shape=[jax.ShapeDtypeStruct((slots, model_width - SPLIT), bf)] * rows_y,
        in_specs=[VMEM] * rows_z,
        out_specs=[VMEM] * rows_y,
        compiler_params=SMALL,
        cost_estimate=cost(rows_y * rows_z * slots * (model_width - SPLIT)),
        name="sum_z",
    )(out_b[0], *arrived_b)
    moved_b = [pass_on(tiles_b[k], Y, -k) for k in range(1, rows_y)]
    slot_home = pl.pallas_call(
        functools.partial(last_kernel, rows_z),
        out_shape=jax.ShapeDtypeStruct((slots, model_width + LANES), bf),
        in_specs=[VMEM] * (rows_z + rows_y),
        out_specs=VMEM,
        compiler_params=SMALL,
        cost_estimate=cost(rows_z * slots * wide),
        name="sum_home",
    )(tiles_a[0], *moved_a, tiles_b[0], *moved_b)
    grad_down = lax.dot_general(
        hidden, scaled, LEADING, preferred_element_type=jnp.float32
    ).astype(bf)
    grad_gate = lax.dot_general(
        gate_pre_grad, gathered, LEADING, preferred_element_type=jnp.float32
    ).astype(bf)
    grad_up = lax.dot_general(
        up_pre_grad, gathered, LEADING, preferred_element_type=jnp.float32
    ).astype(bf)
    slot_back = lax.all_to_all(
        slot_home.reshape(owners, capacity, model_width + LANES), "expert", 0, 0, tiled=True
    ).reshape(slots, model_width + LANES)
    input_grad = jnp.dot(
        dispatch, slot_back[:, :model_width], preferred_element_type=jnp.float32
    ).astype(bf)
    returned = joined(slot_back[:, model_width:])
    product = jnp.sum(token_hot * returned[None, None, :, 0], axis=2)
    gate_grad = product / gates
    return (gate_grad, input_grad, grad_gate[None], grad_up[None], grad_down[None])


def solution(mesh):
    torus = Mesh(
        mesh.devices.reshape(mesh.shape["expert"], 4, 8), ("expert", "replica_0", "replica_1")
    )
    in_specs = (
        P(EXPERT_REPLICA, None),
        P(EXPERT_REPLICA, None),
        P(EXPERT_REPLICA, None),
        P(EXPERT_REPLICA, None),
        P("expert", REPLICA, None),
        P("expert", REPLICA, None),
        P("expert", REPLICA, None),
    )
    out_specs = (
        P(EXPERT_REPLICA, None),
        P(EXPERT_REPLICA, None),
        P("expert", REPLICA, None),
        P("expert", REPLICA, None),
        P("expert", REPLICA, None),
    )

    return jax.shard_map(
        on_device, mesh=torus, in_specs=in_specs, out_specs=out_specs, check_vma=False
    )
```

```python
import functools

import jax
import jax.numpy as jnp
from jax import lax
from jax.experimental import pallas as pl
from jax.experimental.pallas import tpu as pltpu
from jax.sharding import Mesh
from jax.sharding import PartitionSpec as P


REPLICA = ("replica_0", "replica_1")
EXPERT_REPLICA = ("expert", "replica_0", "replica_1")
Y = "replica_0"
Z = "replica_1"
LANES = 128
SPLIT = 2560
CHUNK = 512
VMEM = pl.BlockSpec(memory_space=pltpu.VMEM)
SMEM = pl.BlockSpec(memory_space=pltpu.SMEM)
LIMIT = pltpu.CompilerParams(vmem_limit_bytes=16 * 1024 * 1024)
SMALL = pltpu.CompilerParams(vmem_limit_bytes=8 * 1024 * 1024)
CONTRACT = (((1,), (1,)), ((), ()))
LEADING = (((0,), (0,)), ((), ()))


def pass_on(value, axis, back):
    peers = lax.axis_size(axis)
    return lax.ppermute(value, axis, [((i + back) % peers, i) for i in range(peers)])


def direct(value, axis):
    return [value] + [pass_on(value, axis, k) for k in range(1, lax.axis_size(axis))]


def ring(value, axis, split=True):
    middle = lax.axis_size(axis) // 2
    half = value.shape[0] // 2
    ahead = [pass_on(value, axis, 1)]
    behind = [pass_on(value, axis, -1)]
    for _ in range(middle - 2):
        ahead.append(pass_on(ahead[-1], axis, 1))
        behind.append(pass_on(behind[-1], axis, -1))
    if not split:
        return [value] + ahead + [pass_on(ahead[-1], axis, 1)] + behind[::-1]
    first = pass_on(ahead[-1][:half], axis, 1)
    last = pass_on(behind[-1][half:], axis, -1)
    return [value] + ahead + [first, last] + behind[::-1]


def far_first(peers):
    return sorted(range(1, peers), key=lambda k: -min(k, peers - k))


def high_low(value):
    high = value.astype(jnp.bfloat16)
    low = (value - high.astype(jnp.float32)).astype(jnp.bfloat16)
    lane = lax.broadcasted_iota(jnp.int32, (value.shape[0], LANES), 1)
    both = jnp.where(
        lane == 0,
        high.astype(jnp.float32),
        jnp.where(lane == 1, low.astype(jnp.float32), jnp.float32(0)),
    )
    return both.astype(jnp.bfloat16)


def joined(columns):
    return jnp.sum(columns.astype(jnp.float32), axis=1, keepdims=True)


def main_kernel(rows_y, rows_z, slots, count_t, count_s, *refs):
    token_refs, refs = refs[:count_t], refs[count_t:]
    scaled_refs, refs = refs[:count_s], refs[count_s:]
    wg, wu, wd, t_all, s_all, hid_s, gpg_t, upg_t = refs[:8]
    refs = refs[8:]
    out_a, refs = refs[:rows_y], refs[rows_y:]
    out_b, refs = refs[:rows_z], refs[rows_z:]
    acc_g, acc_u, acc_h, val_s, gpg_s, upg_s = refs
    width = t_all.shape[1]
    total = rows_y * rows_z * slots
    acc_g[...] = jnp.zeros_like(acc_g)
    acc_u[...] = jnp.zeros_like(acc_u)
    acc_h[...] = jnp.zeros_like(acc_h)

    def forward(step, carry):
        cols = pl.ds(pl.multiple_of(step * CHUNK, CHUNK), CHUNK)
        for blocks, whole in ((token_refs, t_all), (scaled_refs, s_all)):
            row = 0
            for block in blocks:
                whole[row : row + block.shape[0], cols] = block[:, cols]
                row += block.shape[0]
        rows_t = t_all[:, cols]
        acc_g[...] += lax.dot_general(
            rows_t, wg[:, cols], CONTRACT, preferred_element_type=jnp.float32
        )
        acc_u[...] += lax.dot_general(
            rows_t, wu[:, cols], CONTRACT, preferred_element_type=jnp.float32
        )
        acc_h[...] += lax.dot_general(
            s_all[:, cols], wd[:, cols], CONTRACT, preferred_element_type=jnp.float32
        )
        return carry

    lax.fori_loop(0, width // CHUNK, forward, 0)

    def middle(dz, carry):
        for dy in range(rows_y):
            here = pl.ds(pl.multiple_of((dy * rows_z + dz) * slots, slots), slots)
            there = pl.ds(pl.multiple_of((dz * rows_y + dy) * slots, slots), slots)
            gate_pre = acc_g[here, :]
            up_pre = acc_u[here, :]
            hidden_grad = acc_h[there, :]
            sigmoid_gate = jax.nn.sigmoid(gate_pre)
            active = gate_pre * sigmoid_gate
            hidden = (active * up_pre).astype(jnp.bfloat16)
            val_s[here, :] = high_low(
                jnp.sum(hidden.astype(jnp.float32) * hidden_grad, axis=1, keepdims=True)
            )
            gate_grad = (
                hidden_grad * up_pre * sigmoid_gate * (1.0 + gate_pre * (1.0 - sigmoid_gate))
            ).astype(jnp.bfloat16)
            up_grad = (hidden_grad * active).astype(jnp.bfloat16)
            hid_s[there, :] = hidden
            gpg_t[here, :] = gate_grad
            upg_t[here, :] = up_grad
            gpg_s[there, :] = gate_grad
            upg_s[there, :] = up_grad
        return carry

    lax.fori_loop(0, rows_z, middle, 0, unroll=2)

    def slots_of(left, right, outs, shift):
        rows = total // len(outs)

        def step_of(step, carry):
            cols = pl.ds(pl.multiple_of(step * CHUNK, CHUNK), CHUNK)
            wide = pl.ds(pl.multiple_of(step * CHUNK + shift, CHUNK), CHUNK)
            value = (
                jnp.dot(left[...], wg[:, wide], preferred_element_type=jnp.float32)
                + jnp.dot(right[...], wu[:, wide], preferred_element_type=jnp.float32)
            ).astype(jnp.bfloat16)
            for k, out in enumerate(outs):
                out[:, cols] = value[k * rows : (k + 1) * rows]
            return carry

        return step_of

    lax.fori_loop(0, SPLIT // CHUNK, slots_of(gpg_t, upg_t, out_a, 0), 0)
    for k, out in enumerate(out_a):
        rows = total // rows_y
        out[:, SPLIT:] = val_s[k * rows : (k + 1) * rows, :]
    lax.fori_loop(0, (width - SPLIT) // CHUNK, slots_of(gpg_s, upg_s, out_b, SPLIT), 0)


def main_call(token_blocks, scaled_blocks, wg, wu, wd, rows_y, rows_z, slots):
    total = rows_y * rows_z * slots
    hidden, width = wg.shape
    bf = jnp.bfloat16
    shapes = [jax.ShapeDtypeStruct((total, width), bf)] * 2
    shapes += [jax.ShapeDtypeStruct((total, hidden), bf)] * 3
    shapes += [jax.ShapeDtypeStruct((total // rows_y, SPLIT + LANES), bf)] * rows_y
    shapes += [jax.ShapeDtypeStruct((total // rows_z, width - SPLIT), bf)] * rows_z
    blocks = list(token_blocks) + list(scaled_blocks)
    outs = pl.pallas_call(
        functools.partial(
            main_kernel, rows_y, rows_z, slots, len(token_blocks), len(scaled_blocks)
        ),
        out_shape=shapes,
        in_specs=[VMEM] * (len(blocks) + 3),
        out_specs=[VMEM] * len(shapes),
        scratch_shapes=[pltpu.VMEM((total, hidden), jnp.float32)] * 3
        + [pltpu.VMEM((total, LANES), bf)]
        + [pltpu.VMEM((total, hidden), bf)] * 2,
        compiler_params=LIMIT,
        cost_estimate=pl.CostEstimate(
            flops=10 * total * hidden * width, bytes_accessed=30 << 20, transcendentals=0
        ),
        name="experts",
    )(*blocks, wg, wu, wd)
    return outs[:5], outs[5 : 5 + rows_y], outs[5 + rows_y :]


def add_narrow(ins, rows, out):
    value = joined(ins[0][rows, SPLIT:])
    for ref in ins[1:]:
        value = value + joined(ref[rows, SPLIT:])
    out[:, SPLIT:] = high_low(value)


def sum_a_kernel(slots, *refs):
    outs = refs[-(refs[0].shape[0] // slots) :]
    ins = refs[: len(refs) - len(outs)]

    def step(index, carry):
        cols = pl.ds(pl.multiple_of(index * LANES, LANES), LANES)
        for k, out in enumerate(outs):
            rows = slice(k * slots, (k + 1) * slots)
            total = ins[0][rows, cols].astype(jnp.float32)
            for ref in ins[1:]:
                total = total + ref[rows, cols].astype(jnp.float32)
            out[:, cols] = total.astype(jnp.bfloat16)
        return carry

    lax.fori_loop(0, SPLIT // LANES, step, 0)
    for k, out in enumerate(outs):
        add_narrow(ins, slice(k * slots, (k + 1) * slots), out)


def sum_b_kernel(slots, place, *refs):
    ins, out = refs[:-1], refs[-1]
    peers, owners, capacity = out.shape[0], out.shape[1], out.shape[2]

    def step(k, carry):
        rows = pl.ds(pl.multiple_of(k * slots, slots), slots)
        target = lax.rem(place[0] + k, peers)
        total = ins[0][rows, :].astype(jnp.float32)
        for ref in ins[1:]:
            total = total + ref[rows, :].astype(jnp.float32)
        total = total.astype(jnp.bfloat16)
        for e in range(owners):
            out[target, e] = total[e * capacity : (e + 1) * capacity]
        return carry

    lax.fori_loop(0, peers, step, 0)


def last_kernel(*refs):
    ins, out = refs[:-1], refs[-1]

    def step(index, carry):
        cols = pl.ds(pl.multiple_of(index * CHUNK, CHUNK), CHUNK)
        total = ins[0][:, cols].astype(jnp.float32)
        for ref in ins[1:]:
            total = total + ref[:, cols].astype(jnp.float32)
        out[:, cols] = total.astype(jnp.bfloat16)
        return carry

    lax.fori_loop(0, SPLIT // CHUNK, step, 0)
    add_narrow(ins, slice(None), out)


def cost(count):
    return pl.CostEstimate(flops=count, bytes_accessed=3 * count, transcendentals=0)


def on_device(tokens, out_grad, expert_ids, gates, w_gate, w_up, w_down):
    token_count = tokens.shape[0]
    fan_out = expert_ids.shape[1]
    model_width = tokens.shape[1]
    owners = lax.axis_size("expert")
    rows_y = lax.axis_size(Y)
    rows_z = lax.axis_size(Z)
    capacity = max(2, 4 * token_count * fan_out // (3 * owners))
    slots = owners * capacity
    bf = jnp.bfloat16
    flat_ids = expert_ids.reshape(-1)
    sequence_pos = jnp.arange(token_count * fan_out, dtype=jnp.int32)
    earlier = sequence_pos[None, :] < sequence_pos[:, None]
    same_expert = flat_ids[:, None] == flat_ids[None, :]
    slot_rank = jnp.sum(jnp.logical_and(same_expert, earlier), axis=1)
    target = flat_ids * capacity + slot_rank
    token_hot = (target[:, None] == jnp.arange(slots, dtype=jnp.int32)[None, :]).astype(jnp.float32)
    token_hot = token_hot.reshape(token_count, fan_out, slots)
    dispatch = jnp.sum(token_hot, axis=1).astype(bf)
    slot_gate = jnp.sum(token_hot * gates[:, :, None], axis=(0, 1))
    picked = lax.dot_general(
        dispatch,
        jnp.concatenate([tokens, out_grad], axis=1),
        LEADING,
        preferred_element_type=jnp.float32,
    )
    scale = jnp.concatenate(
        [
            jnp.ones((slots, model_width), jnp.float32),
            jnp.broadcast_to(slot_gate[:, None], (slots, model_width)),
        ],
        axis=1,
    )
    send = (picked * scale).astype(bf)
    owned = lax.all_to_all(
        send.reshape(owners, capacity, 2 * model_width), "expert", 0, 0, tiled=True
    ).reshape(slots, 2 * model_width)
    owned, place = lax.optimization_barrier((owned, lax.axis_index(Y).reshape(1)))
    scaled_y = jnp.concatenate(direct(owned[:, model_width:], Y), axis=0)
    tokens_z = jnp.concatenate(
        ring(owned[:, :model_width], Z, split=False), axis=0
    )
    token_blocks = ring(tokens_z, Y)
    scaled_blocks = ring(scaled_y, Z)
    (gathered, scaled, hidden, gate_pre_grad, up_pre_grad), out_a, out_b = main_call(
        token_blocks, scaled_blocks, w_gate[0], w_up[0], w_down[0], rows_y, rows_z, slots
    )
    arrived_b = [pass_on(out_b[k], Z, -k) for k in far_first(rows_z)]
    arrived_a = [pass_on(out_a[k], Y, -k) for k in range(1, rows_y)]
    grad_down = lax.dot_general(
        hidden, scaled, LEADING, preferred_element_type=jnp.float32
    ).astype(bf)
    grad_gate = lax.dot_general(
        gate_pre_grad, gathered, LEADING, preferred_element_type=jnp.float32
    ).astype(bf)
    grad_up = lax.dot_general(
        up_pre_grad, gathered, LEADING, preferred_element_type=jnp.float32
    ).astype(bf)
    wide = SPLIT + LANES
    narrow = model_width - SPLIT
    tiles_b = pl.pallas_call(
        functools.partial(sum_b_kernel, slots),
        out_shape=jax.ShapeDtypeStruct((rows_y, owners, capacity, narrow), bf),
        in_specs=[SMEM] + [VMEM] * rows_z,
        out_specs=VMEM,
        compiler_params=SMALL,
        cost_estimate=cost(rows_y * rows_z * slots * narrow),
        name="sum_z",
    )(place, out_b[0], *arrived_b)
    back_b = lax.all_to_all(
        tiles_b.reshape(rows_y * owners, capacity, narrow), (Y, "expert"), 0, 0, tiled=True
    ).reshape(rows_y * slots, narrow)
    tiles_a = pl.pallas_call(
        functools.partial(sum_a_kernel, slots),
        out_shape=[jax.ShapeDtypeStruct((slots, wide), bf)] * rows_z,
        in_specs=[VMEM] * rows_y,
        out_specs=[VMEM] * rows_z,
        compiler_params=SMALL,
        cost_estimate=cost(rows_y * rows_z * slots * wide),
        name="sum_y",
    )(out_a[0], *arrived_a)
    moved_a = [pass_on(tiles_a[k], Z, -k) for k in far_first(rows_z)]
    slot_home = pl.pallas_call(
        last_kernel,
        out_shape=jax.ShapeDtypeStruct((slots, wide), bf),
        in_specs=[VMEM] * rows_z,
        out_specs=VMEM,
        compiler_params=SMALL,
        cost_estimate=cost(rows_z * slots * wide),
        name="sum_home",
    )(tiles_a[0], *moved_a)
    back_a = lax.all_to_all(
        slot_home.reshape(owners, capacity, wide), "expert", 0, 0, tiled=True
    ).reshape(slots, wide)

    def combine(times, value):
        return jnp.dot(
            jnp.concatenate([dispatch] * times, axis=1), value, preferred_element_type=jnp.float32
        )

    input_grad = jnp.concatenate(
        [combine(1, back_a[:, :SPLIT]), combine(rows_y, back_b)], axis=1
    ).astype(bf)
    returned = joined(back_a[:, SPLIT:])
    product = jnp.sum(token_hot * returned[None, None, :, 0], axis=2)
    gate_grad = product / gates
    return (gate_grad, input_grad, grad_gate[None], grad_up[None], grad_down[None])


def solution(mesh):
    torus = Mesh(
        mesh.devices.reshape(mesh.shape["expert"], 4, 8), ("expert", "replica_0", "replica_1")
    )
    in_specs = (
        P(EXPERT_REPLICA, None),
        P(EXPERT_REPLICA, None),
        P(EXPERT_REPLICA, None),
        P(EXPERT_REPLICA, None),
        P("expert", REPLICA, None),
        P("expert", REPLICA, None),
        P("expert", REPLICA, None),
    )
    out_specs = (
        P(EXPERT_REPLICA, None),
        P(EXPERT_REPLICA, None),
        P("expert", REPLICA, None),
        P("expert", REPLICA, None),
        P("expert", REPLICA, None),
    )

    return jax.shard_map(
        on_device, mesh=torus, in_specs=in_specs, out_specs=out_specs, check_vma=False
    )
```

```python
import functools

import jax
import jax.numpy as jnp
from jax import lax
from jax.experimental import pallas as pl
from jax.experimental.pallas import tpu as pltpu
from jax.sharding import Mesh
from jax.sharding import PartitionSpec as P


REPLICA = ("replica_0", "replica_1")
EXPERT_REPLICA = ("expert", "replica_0", "replica_1")
Y = "replica_0"
Z = "replica_1"
LANES = 128
SPLIT = 2816
CHUNK = 512
STEP = 256
VMEM = pl.BlockSpec(memory_space=pltpu.VMEM)
SMEM = pl.BlockSpec(memory_space=pltpu.SMEM)
LIMIT = pltpu.CompilerParams(vmem_limit_bytes=16 * 1024 * 1024)
SMALL = pltpu.CompilerParams(vmem_limit_bytes=8 * 1024 * 1024)
CONTRACT = (((1,), (1,)), ((), ()))
LEADING = (((0,), (0,)), ((), ()))


def pass_on(value, axis, back):
    peers = lax.axis_size(axis)
    return lax.ppermute(value, axis, [((i + back) % peers, i) for i in range(peers)])


def ring(value, axis, split=True):
    middle = lax.axis_size(axis) // 2
    half = value.shape[0] // 2
    ahead = [pass_on(value, axis, 1)]
    behind = [pass_on(value, axis, -1)]
    for _ in range(middle - 2):
        ahead.append(pass_on(ahead[-1], axis, 1))
        behind.append(pass_on(behind[-1], axis, -1))
    if not split:
        return [value] + ahead + [pass_on(ahead[-1], axis, 1)] + behind[::-1]
    first = pass_on(ahead[-1][:half], axis, 1)
    last = pass_on(behind[-1][half:], axis, -1)
    return [value] + ahead + [first, last] + behind[::-1]


def far_first(peers):
    return sorted(range(1, peers), key=lambda k: -min(k, peers - k))


def high_low(value):
    high = value.astype(jnp.bfloat16)
    low = (value - high.astype(jnp.float32)).astype(jnp.bfloat16)
    lane = lax.broadcasted_iota(jnp.int32, (value.shape[0], LANES), 1)
    both = jnp.where(
        lane == 0,
        high.astype(jnp.float32),
        jnp.where(lane == 1, low.astype(jnp.float32), jnp.float32(0)),
    )
    return both.astype(jnp.bfloat16)


def joined(columns):
    return jnp.sum(columns.astype(jnp.float32), axis=1, keepdims=True)


def main_kernel(rows_y, rows_z, slots, count_t, count_s, place, *refs):
    token_refs, refs = refs[:count_t], refs[count_t:]
    scaled_refs, refs = refs[:count_s], refs[count_s:]
    wg, wu, wd, t_all, s_all, hid_s, gpg_t, upg_t = refs[:8]
    refs = refs[8:]
    out_a, refs = refs[:rows_y], refs[rows_y:]
    out_b, refs = refs[:rows_z], refs[rows_z:]
    acc_g, acc_u, acc_h, val_s, gpg_s, upg_s = refs
    width = t_all.shape[1]
    total = rows_y * rows_z * slots
    acc_g[...] = jnp.zeros_like(acc_g)
    acc_u[...] = jnp.zeros_like(acc_u)
    acc_h[...] = jnp.zeros_like(acc_h)

    def forward(step, carry):
        cols = pl.ds(pl.multiple_of(step * CHUNK, CHUNK), CHUNK)
        for blocks, whole in ((token_refs, t_all), (scaled_refs, s_all)):
            row = 0
            for block in blocks:
                whole[row : row + block.shape[0], cols] = block[:, cols]
                row += block.shape[0]
        rows_t = t_all[:, cols]
        acc_g[...] += lax.dot_general(
            rows_t, wg[:, cols], CONTRACT, preferred_element_type=jnp.float32
        )
        acc_u[...] += lax.dot_general(
            rows_t, wu[:, cols], CONTRACT, preferred_element_type=jnp.float32
        )
        acc_h[...] += lax.dot_general(
            s_all[:, cols], wd[:, cols], CONTRACT, preferred_element_type=jnp.float32
        )
        return carry

    lax.fori_loop(0, width // CHUNK, forward, 0)

    def middle(dz, carry):
        for dy in range(rows_y):
            here = pl.ds(pl.multiple_of((dy * rows_z + dz) * slots, slots), slots)
            at_y = lax.rem(place[0] + dy, rows_y)
            there = pl.ds(pl.multiple_of((dz * rows_y + at_y) * slots, slots), slots)
            gate_pre = acc_g[here, :]
            up_pre = acc_u[here, :]
            hidden_grad = acc_h[there, :]
            sigmoid_gate = jax.nn.sigmoid(gate_pre)
            active = gate_pre * sigmoid_gate
            hidden = (active * up_pre).astype(jnp.bfloat16)
            val_s[here, :] = high_low(
                jnp.sum(hidden.astype(jnp.float32) * hidden_grad, axis=1, keepdims=True)
            )
            gate_grad = (
                hidden_grad * up_pre * sigmoid_gate * (1.0 + gate_pre * (1.0 - sigmoid_gate))
            ).astype(jnp.bfloat16)
            up_grad = (hidden_grad * active).astype(jnp.bfloat16)
            hid_s[there, :] = hidden
            gpg_t[here, :] = gate_grad
            upg_t[here, :] = up_grad
            gpg_s[there, :] = gate_grad
            upg_s[there, :] = up_grad
        return carry

    lax.fori_loop(0, rows_z, middle, 0, unroll=2)

    def slots_of(left, right, outs, shift):
        rows = total // len(outs)

        def step_of(step, carry):
            cols = pl.ds(pl.multiple_of(step * STEP, STEP), STEP)
            wide = pl.ds(pl.multiple_of(step * STEP + shift, STEP), STEP)
            value = (
                jnp.dot(left[...], wg[:, wide], preferred_element_type=jnp.float32)
                + jnp.dot(right[...], wu[:, wide], preferred_element_type=jnp.float32)
            ).astype(jnp.bfloat16)
            for k, out in enumerate(outs):
                out[:, cols] = value[k * rows : (k + 1) * rows]
            return carry

        return step_of

    lax.fori_loop(0, SPLIT // STEP, slots_of(gpg_t, upg_t, out_a, 0), 0)
    for k, out in enumerate(out_a):
        rows = total // rows_y
        out[:, SPLIT:] = val_s[k * rows : (k + 1) * rows, :]
    lax.fori_loop(0, (width - SPLIT) // STEP, slots_of(gpg_s, upg_s, out_b, SPLIT), 0)


def main_call(place, token_blocks, scaled_blocks, wg, wu, wd, rows_y, rows_z, slots):
    total = rows_y * rows_z * slots
    hidden, width = wg.shape
    bf = jnp.bfloat16
    shapes = [jax.ShapeDtypeStruct((total, width), bf)] * 2
    shapes += [jax.ShapeDtypeStruct((total, hidden), bf)] * 3
    shapes += [jax.ShapeDtypeStruct((total // rows_y, SPLIT + LANES), bf)] * rows_y
    shapes += [jax.ShapeDtypeStruct((total // rows_z, width - SPLIT), bf)] * rows_z
    blocks = list(token_blocks) + list(scaled_blocks)
    outs = pl.pallas_call(
        functools.partial(
            main_kernel, rows_y, rows_z, slots, len(token_blocks), len(scaled_blocks)
        ),
        out_shape=shapes,
        in_specs=[SMEM] + [VMEM] * (len(blocks) + 3),
        out_specs=[VMEM] * len(shapes),
        scratch_shapes=[pltpu.VMEM((total, hidden), jnp.float32)] * 3
        + [pltpu.VMEM((total, LANES), bf)]
        + [pltpu.VMEM((total, hidden), bf)] * 2,
        compiler_params=LIMIT,
        cost_estimate=pl.CostEstimate(
            flops=10 * total * hidden * width, bytes_accessed=30 << 20, transcendentals=0
        ),
        name="experts",
    )(place, *blocks, wg, wu, wd)
    return outs[:5], outs[5 : 5 + rows_y], outs[5 + rows_y :]


def add_narrow(ins, rows, out):
    value = joined(ins[0][rows, SPLIT:])
    for ref in ins[1:]:
        value = value + joined(ref[rows, SPLIT:])
    out[:, SPLIT:] = high_low(value)


def sum_a_kernel(slots, *refs):
    outs = refs[-(refs[0].shape[0] // slots) :]
    ins = refs[: len(refs) - len(outs)]

    def step(index, carry):
        cols = pl.ds(pl.multiple_of(index * LANES, LANES), LANES)
        for k, out in enumerate(outs):
            rows = slice(k * slots, (k + 1) * slots)
            total = ins[0][rows, cols].astype(jnp.float32)
            for ref in ins[1:]:
                total = total + ref[rows, cols].astype(jnp.float32)
            out[:, cols] = total.astype(jnp.bfloat16)
        return carry

    lax.fori_loop(0, SPLIT // LANES, step, 0)
    for k, out in enumerate(outs):
        add_narrow(ins, slice(k * slots, (k + 1) * slots), out)


def sum_b_kernel(slots, *refs):
    ins, out = refs[:-1], refs[-1]
    peers, owners, capacity = out.shape[0], out.shape[1], out.shape[2]

    def step(k, carry):
        rows = pl.ds(pl.multiple_of(k * slots, slots), slots)
        total = ins[0][rows, :].astype(jnp.float32)
        for ref in ins[1:]:
            total = total + ref[rows, :].astype(jnp.float32)
        total = total.astype(jnp.bfloat16)
        for e in range(owners):
            out[k, e] = total[e * capacity : (e + 1) * capacity]
        return carry

    lax.fori_loop(0, peers, step, 0)


def last_kernel(*refs):
    ins, out = refs[:-1], refs[-1]

    def step(index, carry):
        cols = pl.ds(pl.multiple_of(index * STEP, STEP), STEP)
        total = ins[0][:, cols].astype(jnp.float32)
        for ref in ins[1:]:
            total = total + ref[:, cols].astype(jnp.float32)
        out[:, cols] = total.astype(jnp.bfloat16)
        return carry

    lax.fori_loop(0, SPLIT // STEP, step, 0)
    add_narrow(ins, slice(None), out)


def cost(count):
    return pl.CostEstimate(flops=count, bytes_accessed=3 * count, transcendentals=0)


def on_device(tokens, out_grad, expert_ids, gates, w_gate, w_up, w_down):
    token_count = tokens.shape[0]
    fan_out = expert_ids.shape[1]
    model_width = tokens.shape[1]
    owners = lax.axis_size("expert")
    rows_y = lax.axis_size(Y)
    rows_z = lax.axis_size(Z)
    capacity = max(2, 4 * token_count * fan_out // (3 * owners))
    slots = owners * capacity
    bf = jnp.bfloat16
    flat_ids = expert_ids.reshape(-1)
    sequence_pos = jnp.arange(token_count * fan_out, dtype=jnp.int32)
    earlier = sequence_pos[None, :] < sequence_pos[:, None]
    same_expert = flat_ids[:, None] == flat_ids[None, :]
    slot_rank = jnp.sum(jnp.logical_and(same_expert, earlier), axis=1)
    target = flat_ids * capacity + slot_rank
    token_hot = (target[:, None] == jnp.arange(slots, dtype=jnp.int32)[None, :]).astype(jnp.float32)
    token_hot = token_hot.reshape(token_count, fan_out, slots)
    dispatch = jnp.sum(token_hot, axis=1).astype(bf)
    slot_gate = jnp.sum(token_hot * gates[:, :, None], axis=(0, 1))
    send_tokens = lax.dot_general(dispatch, tokens, LEADING, preferred_element_type=jnp.float32)
    send_scaled = slot_gate[:, None] * lax.dot_general(
        dispatch, out_grad, LEADING, preferred_element_type=jnp.float32
    )
    owned = lax.all_to_all(
        send_tokens.astype(bf).reshape(owners, capacity, model_width),
        "expert",
        0,
        0,
        tiled=True,
    ).reshape(slots, model_width)
    copies = jnp.broadcast_to(
        send_scaled.astype(bf).reshape(1, owners, capacity, model_width),
        (rows_y, owners, capacity, model_width),
    ).reshape(rows_y * owners, capacity, model_width)
    copies, place = lax.optimization_barrier((copies, lax.axis_index(Y).reshape(1)))
    scaled_y = lax.all_to_all(copies, (Y, "expert"), 0, 0, tiled=True).reshape(
        rows_y * slots, model_width
    )
    tokens_z = jnp.concatenate(ring(owned, Z, split=False), axis=0)
    token_blocks = ring(tokens_z, Y)
    scaled_blocks = ring(scaled_y, Z)
    (gathered, scaled, hidden, gate_pre_grad, up_pre_grad), out_a, out_b = main_call(
        place, token_blocks, scaled_blocks, w_gate[0], w_up[0], w_down[0], rows_y, rows_z, slots
    )
    arrived_b = [pass_on(out_b[k], Z, -k) for k in far_first(rows_z)]
    arrived_a = [pass_on(out_a[k], Y, -k) for k in range(1, rows_y)]
    grad_down = lax.dot_general(
        hidden, scaled, LEADING, preferred_element_type=jnp.float32
    ).astype(bf)
    grad_gate = lax.dot_general(
        gate_pre_grad, gathered, LEADING, preferred_element_type=jnp.float32
    ).astype(bf)
    grad_up = lax.dot_general(
        up_pre_grad, gathered, LEADING, preferred_element_type=jnp.float32
    ).astype(bf)
    wide = SPLIT + LANES
    narrow = model_width - SPLIT
    tiles_b = pl.pallas_call(
        functools.partial(sum_b_kernel, slots),
        out_shape=jax.ShapeDtypeStruct((rows_y, owners, capacity, narrow), bf),
        in_specs=[VMEM] * rows_z,
        out_specs=VMEM,
        compiler_params=SMALL,
        cost_estimate=cost(rows_y * rows_z * slots * narrow),
        name="sum_z",
    )(out_b[0], *arrived_b)
    back_b = lax.all_to_all(
        tiles_b.reshape(rows_y * owners, capacity, narrow), (Y, "expert"), 0, 0, tiled=True
    ).reshape(rows_y * slots, narrow)
    tiles_a = pl.pallas_call(
        functools.partial(sum_a_kernel, slots),
        out_shape=[jax.ShapeDtypeStruct((slots, wide), bf)] * rows_z,
        in_specs=[VMEM] * rows_y,
        out_specs=[VMEM] * rows_z,
        compiler_params=SMALL,
        cost_estimate=cost(rows_y * rows_z * slots * wide),
        name="sum_y",
    )(out_a[0], *arrived_a)
    moved_a = [pass_on(tiles_a[k], Z, -k) for k in far_first(rows_z)]
    slot_home = pl.pallas_call(
        last_kernel,
        out_shape=jax.ShapeDtypeStruct((slots, wide), bf),
        in_specs=[VMEM] * rows_z,
        out_specs=VMEM,
        compiler_params=SMALL,
        cost_estimate=cost(rows_z * slots * wide),
        name="sum_home",
    )(tiles_a[0], *moved_a)
    back_a = lax.all_to_all(
        slot_home.reshape(owners, capacity, wide), "expert", 0, 0, tiled=True
    ).reshape(slots, wide)

    def combine(times, value):
        return jnp.dot(
            jnp.concatenate([dispatch] * times, axis=1), value, preferred_element_type=jnp.float32
        )

    input_grad = jnp.concatenate(
        [combine(1, back_a[:, :SPLIT]), combine(rows_y, back_b)], axis=1
    ).astype(bf)
    returned = joined(back_a[:, SPLIT:])
    product = jnp.sum(token_hot * returned[None, None, :, 0], axis=2)
    gate_grad = product / gates
    return (gate_grad, input_grad, grad_gate[None], grad_up[None], grad_down[None])


def solution(mesh):
    torus = Mesh(
        mesh.devices.reshape(mesh.shape["expert"], 4, 8), ("expert", "replica_0", "replica_1")
    )
    in_specs = (
        P(EXPERT_REPLICA, None),
        P(EXPERT_REPLICA, None),
        P(EXPERT_REPLICA, None),
        P(EXPERT_REPLICA, None),
        P("expert", REPLICA, None),
        P("expert", REPLICA, None),
        P("expert", REPLICA, None),
    )
    out_specs = (
        P(EXPERT_REPLICA, None),
        P(EXPERT_REPLICA, None),
        P("expert", REPLICA, None),
        P("expert", REPLICA, None),
        P("expert", REPLICA, None),
    )

    return jax.shard_map(
        on_device, mesh=torus, in_specs=in_specs, out_specs=out_specs, check_vma=False
    )
```

```python
import functools

import jax
import jax.numpy as jnp
from jax import lax
from jax.experimental import pallas as pl
from jax.experimental.pallas import tpu as pltpu
from jax.sharding import Mesh
from jax.sharding import PartitionSpec as P


REPLICA = ("replica_0", "replica_1")
EXPERT_REPLICA = ("expert", "replica_0", "replica_1")
Y = "replica_0"
Z = "replica_1"
LANES = 128
SPLIT = 2560
CHUNK = 512
STEP = 512
VMEM = pl.BlockSpec(memory_space=pltpu.VMEM)
SMEM = pl.BlockSpec(memory_space=pltpu.SMEM)
LIMIT = pltpu.CompilerParams(vmem_limit_bytes=16 * 1024 * 1024)
SMALL = pltpu.CompilerParams(vmem_limit_bytes=8 * 1024 * 1024)
CONTRACT = (((1,), (1,)), ((), ()))
LEADING = (((0,), (0,)), ((), ()))


def pass_on(value, axis, back):
    peers = lax.axis_size(axis)
    return lax.ppermute(value, axis, [((i + back) % peers, i) for i in range(peers)])


def ring(value, axis, split=True):
    middle = lax.axis_size(axis) // 2
    half = value.shape[0] // 2
    ahead = [pass_on(value, axis, 1)]
    behind = [pass_on(value, axis, -1)]
    for _ in range(middle - 2):
        ahead.append(pass_on(ahead[-1], axis, 1))
        behind.append(pass_on(behind[-1], axis, -1))
    if not split:
        return [value] + ahead + [pass_on(ahead[-1], axis, 1)] + behind[::-1]
    first = pass_on(ahead[-1][:half], axis, 1)
    last = pass_on(behind[-1][half:], axis, -1)
    return [value] + ahead + [first, last] + behind[::-1]


def far_first(peers):
    return sorted(range(1, peers), key=lambda k: -min(k, peers - k))


def high_low(value):
    high = value.astype(jnp.bfloat16)
    low = (value - high.astype(jnp.float32)).astype(jnp.bfloat16)
    lane = lax.broadcasted_iota(jnp.int32, (value.shape[0], LANES), 1)
    both = jnp.where(
        lane == 0,
        high.astype(jnp.float32),
        jnp.where(lane == 1, low.astype(jnp.float32), jnp.float32(0)),
    )
    return both.astype(jnp.bfloat16)


def joined(columns):
    return jnp.sum(columns.astype(jnp.float32), axis=1, keepdims=True)


def main_kernel(rows_y, rows_z, slots, count_t, count_s, place, *refs):
    token_refs, refs = refs[:count_t], refs[count_t:]
    scaled_refs, refs = refs[:count_s], refs[count_s:]
    wg, wu, wd, t_all, s_all, hid_s, gpg_t, upg_t = refs[:8]
    refs = refs[8:]
    out_a, refs = refs[:rows_y], refs[rows_y:]
    out_b, refs = refs[:rows_z], refs[rows_z:]
    acc_g, acc_u, acc_h, val_s, gpg_s, upg_s = refs
    width = t_all.shape[1]
    total = rows_y * rows_z * slots
    acc_g[...] = jnp.zeros_like(acc_g)
    acc_u[...] = jnp.zeros_like(acc_u)
    acc_h[...] = jnp.zeros_like(acc_h)

    def forward(step, carry):
        cols = pl.ds(pl.multiple_of(step * CHUNK, CHUNK), CHUNK)
        for blocks, whole in ((token_refs, t_all), (scaled_refs, s_all)):
            row = 0
            for block in blocks:
                whole[row : row + block.shape[0], cols] = block[:, cols]
                row += block.shape[0]
        rows_t = t_all[:, cols]
        acc_g[...] += lax.dot_general(
            rows_t, wg[:, cols], CONTRACT, preferred_element_type=jnp.float32
        )
        acc_u[...] += lax.dot_general(
            rows_t, wu[:, cols], CONTRACT, preferred_element_type=jnp.float32
        )
        acc_h[...] += lax.dot_general(
            s_all[:, cols], wd[:, cols], CONTRACT, preferred_element_type=jnp.float32
        )
        return carry

    lax.fori_loop(0, width // CHUNK, forward, 0)

    def middle(dz, carry):
        for dy in range(rows_y):
            here = pl.ds(pl.multiple_of((dy * rows_z + dz) * slots, slots), slots)
            at_y = lax.rem(place[0] + dy, rows_y)
            there = pl.ds(pl.multiple_of((dz * rows_y + at_y) * slots, slots), slots)
            gate_pre = acc_g[here, :]
            up_pre = acc_u[here, :]
            hidden_grad = acc_h[there, :]
            sigmoid_gate = jax.nn.sigmoid(gate_pre)
            active = gate_pre * sigmoid_gate
            hidden = (active * up_pre).astype(jnp.bfloat16)
            val_s[here, :] = high_low(
                jnp.sum(hidden.astype(jnp.float32) * hidden_grad, axis=1, keepdims=True)
            )
            gate_grad = (
                hidden_grad * up_pre * sigmoid_gate * (1.0 + gate_pre * (1.0 - sigmoid_gate))
            ).astype(jnp.bfloat16)
            up_grad = (hidden_grad * active).astype(jnp.bfloat16)
            hid_s[there, :] = hidden
            gpg_t[here, :] = gate_grad
            upg_t[here, :] = up_grad
            gpg_s[there, :] = gate_grad
            upg_s[there, :] = up_grad
        return carry

    lax.fori_loop(0, rows_z, middle, 0, unroll=4)

    def slots_of(left, right, outs, shift):
        rows = total // len(outs)

        def step_of(step, carry):
            cols = pl.ds(pl.multiple_of(step * STEP, STEP), STEP)
            wide = pl.ds(pl.multiple_of(step * STEP + shift, STEP), STEP)
            value = (
                jnp.dot(left[...], wg[:, wide], preferred_element_type=jnp.float32)
                + jnp.dot(right[...], wu[:, wide], preferred_element_type=jnp.float32)
            ).astype(jnp.bfloat16)
            for k, out in enumerate(outs):
                out[:, cols] = value[k * rows : (k + 1) * rows]
            return carry

        return step_of

    lax.fori_loop(0, SPLIT // STEP, slots_of(gpg_t, upg_t, out_a, 0), 0)
    for k, out in enumerate(out_a):
        rows = total // rows_y
        out[:, SPLIT:] = val_s[k * rows : (k + 1) * rows, :]
    lax.fori_loop(0, (width - SPLIT) // STEP, slots_of(gpg_s, upg_s, out_b, SPLIT), 0)


def main_call(place, token_blocks, scaled_blocks, wg, wu, wd, rows_y, rows_z, slots):
    total = rows_y * rows_z * slots
    hidden, width = wg.shape
    bf = jnp.bfloat16
    shapes = [jax.ShapeDtypeStruct((total, width), bf)] * 2
    shapes += [jax.ShapeDtypeStruct((total, hidden), bf)] * 3
    shapes += [jax.ShapeDtypeStruct((total // rows_y, SPLIT + LANES), bf)] * rows_y
    shapes += [jax.ShapeDtypeStruct((total // rows_z, width - SPLIT), bf)] * rows_z
    blocks = list(token_blocks) + list(scaled_blocks)
    outs = pl.pallas_call(
        functools.partial(
            main_kernel, rows_y, rows_z, slots, len(token_blocks), len(scaled_blocks)
        ),
        out_shape=shapes,
        in_specs=[SMEM] + [VMEM] * (len(blocks) + 3),
        out_specs=[VMEM] * len(shapes),
        scratch_shapes=[pltpu.VMEM((total, hidden), jnp.float32)] * 3
        + [pltpu.VMEM((total, LANES), bf)]
        + [pltpu.VMEM((total, hidden), bf)] * 2,
        compiler_params=LIMIT,
        cost_estimate=pl.CostEstimate(
            flops=10 * total * hidden * width, bytes_accessed=30 << 20, transcendentals=0
        ),
        name="experts",
    )(place, *blocks, wg, wu, wd)
    return outs[:5], outs[5 : 5 + rows_y], outs[5 + rows_y :]


def add_narrow(ins, rows, out):
    value = joined(ins[0][rows, SPLIT:])
    for ref in ins[1:]:
        value = value + joined(ref[rows, SPLIT:])
    out[:, SPLIT:] = high_low(value)


def touch_kernel(*refs):
    ins, out = refs[:-1], refs[-1]
    total = ins[0][:8, :LANES].astype(jnp.float32)
    for ref in ins[1:]:
        total = total + ref[:8, :LANES].astype(jnp.float32)
    out[...] = total


def touch_call(weights):
    return pl.pallas_call(
        touch_kernel,
        out_shape=jax.ShapeDtypeStruct((8, LANES), jnp.float32),
        in_specs=[VMEM] * len(weights),
        out_specs=VMEM,
        compiler_params=pltpu.CompilerParams(
            vmem_limit_bytes=8 * 1024 * 1024, has_side_effects=True
        ),
        cost_estimate=cost(1 << 10),
        name="touch_weights",
    )(*weights)


def sum_a_kernel(slots, *refs):
    outs = refs[-(refs[0].shape[0] // slots) :]
    ins = refs[: len(refs) - len(outs)]

    def step(index, carry):
        cols = pl.ds(pl.multiple_of(index * LANES, LANES), LANES)
        for k, out in enumerate(outs):
            rows = slice(k * slots, (k + 1) * slots)
            total = ins[0][rows, cols].astype(jnp.float32)
            for ref in ins[1:]:
                total = total + ref[rows, cols].astype(jnp.float32)
            out[:, cols] = total.astype(jnp.bfloat16)
        return carry

    lax.fori_loop(0, SPLIT // LANES, step, 0)
    for k, out in enumerate(outs):
        add_narrow(ins, slice(k * slots, (k + 1) * slots), out)


def sum_b_kernel(slots, *refs):
    ins, out = refs[:-1], refs[-1]
    peers, owners, capacity = out.shape[0], out.shape[1], out.shape[2]

    def step(k, carry):
        rows = pl.ds(pl.multiple_of(k * slots, slots), slots)
        total = ins[0][rows, :].astype(jnp.float32)
        for ref in ins[1:]:
            total = total + ref[rows, :].astype(jnp.float32)
        total = total.astype(jnp.bfloat16)
        for e in range(owners):
            out[k, e] = total[e * capacity : (e + 1) * capacity]
        return carry

    lax.fori_loop(0, peers, step, 0)


def last_kernel(*refs):
    ins, out = refs[:-1], refs[-1]

    def step(index, carry):
        cols = pl.ds(pl.multiple_of(index * STEP, STEP), STEP)
        total = ins[0][:, cols].astype(jnp.float32)
        for ref in ins[1:]:
            total = total + ref[:, cols].astype(jnp.float32)
        out[:, cols] = total.astype(jnp.bfloat16)
        return carry

    lax.fori_loop(0, SPLIT // STEP, step, 0)
    add_narrow(ins, slice(None), out)


def cost(count):
    return pl.CostEstimate(flops=count, bytes_accessed=3 * count, transcendentals=0)


def on_device(tokens, out_grad, expert_ids, gates, w_gate, w_up, w_down):
    token_count = tokens.shape[0]
    fan_out = expert_ids.shape[1]
    model_width = tokens.shape[1]
    owners = lax.axis_size("expert")
    rows_y = lax.axis_size(Y)
    rows_z = lax.axis_size(Z)
    capacity = max(2, 4 * token_count * fan_out // (3 * owners))
    slots = owners * capacity
    bf = jnp.bfloat16
    flat_ids = expert_ids.reshape(-1)
    sequence_pos = jnp.arange(token_count * fan_out, dtype=jnp.int32)
    earlier = sequence_pos[None, :] < sequence_pos[:, None]
    same_expert = flat_ids[:, None] == flat_ids[None, :]
    slot_rank = jnp.sum(jnp.logical_and(same_expert, earlier), axis=1)
    target = flat_ids * capacity + slot_rank
    token_hot = (target[:, None] == jnp.arange(slots, dtype=jnp.int32)[None, :]).astype(jnp.float32)
    token_hot = token_hot.reshape(token_count, fan_out, slots)
    dispatch = jnp.sum(token_hot, axis=1).astype(bf)
    slot_gate = jnp.sum(token_hot * gates[:, :, None], axis=(0, 1))
    send_tokens = lax.dot_general(dispatch, tokens, LEADING, preferred_element_type=jnp.float32)
    send_scaled = slot_gate[:, None] * lax.dot_general(
        dispatch, out_grad, LEADING, preferred_element_type=jnp.float32
    )
    owned = lax.all_to_all(
        send_tokens.astype(bf).reshape(owners, capacity, model_width),
        "expert",
        0,
        0,
        tiled=True,
    ).reshape(slots, model_width)
    copies = jnp.broadcast_to(
        send_scaled.astype(bf).reshape(1, owners, capacity, model_width),
        (rows_y, owners, capacity, model_width),
    ).reshape(rows_y * owners, capacity, model_width)
    copies, place = lax.optimization_barrier((copies, lax.axis_index(Y).reshape(1)))
    scaled_y = lax.all_to_all(copies, (Y, "expert"), 0, 0, tiled=True).reshape(
        rows_y * slots, model_width
    )
    tokens_z = jnp.concatenate(ring(owned, Z, split=False), axis=0)
    touch_call([w_gate[0], w_up[0], w_down[0]])
    token_blocks = ring(tokens_z, Y)
    scaled_blocks = ring(scaled_y, Z)
    (gathered, scaled, hidden, gate_pre_grad, up_pre_grad), out_a, out_b = main_call(
        place, token_blocks, scaled_blocks, w_gate[0], w_up[0], w_down[0], rows_y, rows_z, slots
    )
    arrived_b = [pass_on(out_b[k], Z, -k) for k in far_first(rows_z)]
    arrived_a = [pass_on(out_a[k], Y, -k) for k in range(1, rows_y)]
    grad_down = lax.dot_general(
        hidden, scaled, LEADING, preferred_element_type=jnp.float32
    ).astype(bf)
    grad_gate = lax.dot_general(
        gate_pre_grad, gathered, LEADING, preferred_element_type=jnp.float32
    ).astype(bf)
    grad_up = lax.dot_general(
        up_pre_grad, gathered, LEADING, preferred_element_type=jnp.float32
    ).astype(bf)
    wide = SPLIT + LANES
    narrow = model_width - SPLIT
    tiles_b = pl.pallas_call(
        functools.partial(sum_b_kernel, slots),
        out_shape=jax.ShapeDtypeStruct((rows_y, owners, capacity, narrow), bf),
        in_specs=[VMEM] * rows_z,
        out_specs=VMEM,
        compiler_params=SMALL,
        cost_estimate=cost(rows_y * rows_z * slots * narrow),
        name="sum_z",
    )(out_b[0], *arrived_b)
    back_b = lax.all_to_all(
        tiles_b.reshape(rows_y * owners, capacity, narrow), (Y, "expert"), 0, 0, tiled=True
    ).reshape(rows_y * slots, narrow)
    tiles_a = pl.pallas_call(
        functools.partial(sum_a_kernel, slots),
        out_shape=[jax.ShapeDtypeStruct((slots, wide), bf)] * rows_z,
        in_specs=[VMEM] * rows_y,
        out_specs=[VMEM] * rows_z,
        compiler_params=SMALL,
        cost_estimate=cost(rows_y * rows_z * slots * wide),
        name="sum_y",
    )(out_a[0], *arrived_a)
    moved_a = [pass_on(tiles_a[k], Z, -k) for k in far_first(rows_z)]
    slot_home = pl.pallas_call(
        last_kernel,
        out_shape=jax.ShapeDtypeStruct((slots, wide), bf),
        in_specs=[VMEM] * rows_z,
        out_specs=VMEM,
        compiler_params=SMALL,
        cost_estimate=cost(rows_z * slots * wide),
        name="sum_home",
    )(tiles_a[0], *moved_a)
    back_a = lax.all_to_all(
        slot_home.reshape(owners, capacity, wide), "expert", 0, 0, tiled=True
    ).reshape(slots, wide)

    def combine(times, value):
        return jnp.dot(
            jnp.concatenate([dispatch] * times, axis=1), value, preferred_element_type=jnp.float32
        )

    input_grad = jnp.concatenate(
        [combine(1, back_a[:, :SPLIT]), combine(rows_y, back_b)], axis=1
    ).astype(bf)
    returned = joined(back_a[:, SPLIT:])
    product = jnp.sum(token_hot * returned[None, None, :, 0], axis=2)
    gate_grad = product / gates
    return (gate_grad, input_grad, grad_gate[None], grad_up[None], grad_down[None])


def solution(mesh):
    torus = Mesh(
        mesh.devices.reshape(mesh.shape["expert"], 4, 8), ("expert", "replica_0", "replica_1")
    )
    in_specs = (
        P(EXPERT_REPLICA, None),
        P(EXPERT_REPLICA, None),
        P(EXPERT_REPLICA, None),
        P(EXPERT_REPLICA, None),
        P("expert", REPLICA, None),
        P("expert", REPLICA, None),
        P("expert", REPLICA, None),
    )
    out_specs = (
        P(EXPERT_REPLICA, None),
        P(EXPERT_REPLICA, None),
        P("expert", REPLICA, None),
        P("expert", REPLICA, None),
        P("expert", REPLICA, None),
    )

    return jax.shard_map(
        on_device, mesh=torus, in_specs=in_specs, out_specs=out_specs, check_vma=False
    )
```

```python
import functools

import jax
import jax.numpy as jnp
from jax import lax
from jax.experimental import pallas as pl
from jax.experimental.pallas import tpu as pltpu
from jax.sharding import Mesh
from jax.sharding import PartitionSpec as P


REPLICA = ("replica_0", "replica_1")
EXPERT_REPLICA = ("expert", "replica_0", "replica_1")
Y = "replica_0"
Z = "replica_1"
LANES = 128
SPLIT = 2560
CHUNK = 512
STEP = 512
VMEM = pl.BlockSpec(memory_space=pltpu.VMEM)
SMEM = pl.BlockSpec(memory_space=pltpu.SMEM)
LIMIT = pltpu.CompilerParams(vmem_limit_bytes=16 * 1024 * 1024)
SMALL = pltpu.CompilerParams(vmem_limit_bytes=8 * 1024 * 1024)
CONTRACT = (((1,), (1,)), ((), ()))
LEADING = (((0,), (0,)), ((), ()))


def pass_on(value, axis, back):
    peers = lax.axis_size(axis)
    return lax.ppermute(value, axis, [((i + back) % peers, i) for i in range(peers)])


def ring(value, axis, split=True):
    middle = lax.axis_size(axis) // 2
    half = value.shape[0] // 2
    ahead = [pass_on(value, axis, 1)]
    behind = [pass_on(value, axis, -1)]
    for _ in range(middle - 2):
        ahead.append(pass_on(ahead[-1], axis, 1))
        behind.append(pass_on(behind[-1], axis, -1))
    if not split:
        return [value] + ahead + [pass_on(ahead[-1], axis, 1)] + behind[::-1]
    first = pass_on(ahead[-1][:half], axis, 1)
    last = pass_on(behind[-1][half:], axis, -1)
    return [value] + ahead + [first, last] + behind[::-1]


def far_first(peers):
    return sorted(range(1, peers), key=lambda k: -min(k, peers - k))


def high_low(value):
    high = value.astype(jnp.bfloat16)
    low = (value - high.astype(jnp.float32)).astype(jnp.bfloat16)
    lane = lax.broadcasted_iota(jnp.int32, (value.shape[0], LANES), 1)
    both = jnp.where(
        lane == 0,
        high.astype(jnp.float32),
        jnp.where(lane == 1, low.astype(jnp.float32), jnp.float32(0)),
    )
    return both.astype(jnp.bfloat16)


def joined(columns):
    return jnp.sum(columns.astype(jnp.float32), axis=1, keepdims=True)


def main_kernel(rows_y, rows_z, slots, count_t, count_s, place, *refs):
    token_refs, refs = refs[:count_t], refs[count_t:]
    scaled_refs, refs = refs[:count_s], refs[count_s:]
    wg, wu, wd, t_all, s_all, hid_s, gpg_t, upg_t = refs[:8]
    refs = refs[8:]
    out_a, refs = refs[:rows_y], refs[rows_y:]
    out_b, refs = refs[:rows_z], refs[rows_z:]
    acc_g, acc_u, acc_h, val_s, gpg_s, upg_s = refs
    width = t_all.shape[1]
    total = rows_y * rows_z * slots
    acc_g[...] = jnp.zeros_like(acc_g)
    acc_u[...] = jnp.zeros_like(acc_u)
    acc_h[...] = jnp.zeros_like(acc_h)

    def forward(step, carry):
        cols = pl.ds(pl.multiple_of(step * CHUNK, CHUNK), CHUNK)
        row = 0
        for block in token_refs:
            t_all[row : row + block.shape[0], cols] = block[:, cols]
            row += block.shape[0]
        tile = 0
        for block in scaled_refs:
            for k in range(block.shape[0] // slots):
                dz, at_y = tile // rows_y, tile % rows_y
                dy = lax.rem(at_y + rows_y - place[0], rows_y)
                rows = pl.ds(pl.multiple_of((dz * rows_y + dy) * slots, slots), slots)
                s_all[rows, cols] = block[k * slots : (k + 1) * slots, cols]
                tile += 1
        rows_t = t_all[:, cols]
        acc_g[...] += lax.dot_general(
            rows_t, wg[:, cols], CONTRACT, preferred_element_type=jnp.float32
        )
        acc_u[...] += lax.dot_general(
            rows_t, wu[:, cols], CONTRACT, preferred_element_type=jnp.float32
        )
        acc_h[...] += lax.dot_general(
            s_all[:, cols], wd[:, cols], CONTRACT, preferred_element_type=jnp.float32
        )
        return carry

    lax.fori_loop(0, width // CHUNK, forward, 0)

    for dz in range(rows_z):
        for dy in range(rows_y):
            here = pl.ds((dy * rows_z + dz) * slots, slots)
            there = pl.ds((dz * rows_y + dy) * slots, slots)
            gate_pre = acc_g[here, :]
            up_pre = acc_u[here, :]
            hidden_grad = acc_h[there, :]
            sigmoid_gate = jax.nn.sigmoid(gate_pre)
            active = gate_pre * sigmoid_gate
            hidden = (active * up_pre).astype(jnp.bfloat16)
            val_s[here, :] = high_low(
                jnp.sum(hidden.astype(jnp.float32) * hidden_grad, axis=1, keepdims=True)
            )
            gate_grad = (
                hidden_grad * up_pre * sigmoid_gate * (1.0 + gate_pre * (1.0 - sigmoid_gate))
            ).astype(jnp.bfloat16)
            up_grad = (hidden_grad * active).astype(jnp.bfloat16)
            hid_s[there, :] = hidden
            gpg_t[here, :] = gate_grad
            upg_t[here, :] = up_grad
            gpg_s[there, :] = gate_grad
            upg_s[there, :] = up_grad

    def slots_of(left, right, outs, shift):
        rows = total // len(outs)

        def step_of(step, carry):
            cols = pl.ds(pl.multiple_of(step * STEP, STEP), STEP)
            wide = pl.ds(pl.multiple_of(step * STEP + shift, STEP), STEP)
            value = (
                jnp.dot(left[...], wg[:, wide], preferred_element_type=jnp.float32)
                + jnp.dot(right[...], wu[:, wide], preferred_element_type=jnp.float32)
            ).astype(jnp.bfloat16)
            for k, out in enumerate(outs):
                out[:, cols] = value[k * rows : (k + 1) * rows]
            return carry

        return step_of

    lax.fori_loop(0, SPLIT // STEP, slots_of(gpg_t, upg_t, out_a, 0), 0)
    for k, out in enumerate(out_a):
        rows = total // rows_y
        out[:, SPLIT:] = val_s[k * rows : (k + 1) * rows, :]
    lax.fori_loop(0, (width - SPLIT) // STEP, slots_of(gpg_s, upg_s, out_b, SPLIT), 0)


def main_call(place, token_blocks, scaled_blocks, wg, wu, wd, rows_y, rows_z, slots):
    total = rows_y * rows_z * slots
    hidden, width = wg.shape
    bf = jnp.bfloat16
    shapes = [jax.ShapeDtypeStruct((total, width), bf)] * 2
    shapes += [jax.ShapeDtypeStruct((total, hidden), bf)] * 3
    shapes += [jax.ShapeDtypeStruct((total // rows_y, SPLIT + LANES), bf)] * rows_y
    shapes += [jax.ShapeDtypeStruct((total // rows_z, width - SPLIT), bf)] * rows_z
    blocks = list(token_blocks) + list(scaled_blocks)
    outs = pl.pallas_call(
        functools.partial(
            main_kernel, rows_y, rows_z, slots, len(token_blocks), len(scaled_blocks)
        ),
        out_shape=shapes,
        in_specs=[SMEM] + [VMEM] * (len(blocks) + 3),
        out_specs=[VMEM] * len(shapes),
        scratch_shapes=[pltpu.VMEM((total, hidden), jnp.float32)] * 3
        + [pltpu.VMEM((total, LANES), bf)]
        + [pltpu.VMEM((total, hidden), bf)] * 2,
        compiler_params=LIMIT,
        cost_estimate=pl.CostEstimate(
            flops=10 * total * hidden * width, bytes_accessed=30 << 20, transcendentals=0
        ),
        name="experts",
    )(place, *blocks, wg, wu, wd)
    return outs[:5], outs[5 : 5 + rows_y], outs[5 + rows_y :]


def add_narrow(ins, rows, out):
    value = joined(ins[0][rows, SPLIT:])
    for ref in ins[1:]:
        value = value + joined(ref[rows, SPLIT:])
    out[:, SPLIT:] = high_low(value)


def touch_kernel(*refs):
    ins, out = refs[:-1], refs[-1]
    total = ins[0][:8, :LANES].astype(jnp.float32)
    for ref in ins[1:]:
        total = total + ref[:8, :LANES].astype(jnp.float32)
    out[...] = total


def touch_call(weights):
    return pl.pallas_call(
        touch_kernel,
        out_shape=jax.ShapeDtypeStruct((8, LANES), jnp.float32),
        in_specs=[VMEM] * len(weights),
        out_specs=VMEM,
        compiler_params=pltpu.CompilerParams(
            vmem_limit_bytes=8 * 1024 * 1024, has_side_effects=True
        ),
        cost_estimate=cost(1 << 10),
        name="touch_weights",
    )(*weights)


def sum_a_kernel(slots, *refs):
    outs = refs[-(refs[0].shape[0] // slots) :]
    ins = refs[: len(refs) - len(outs)]

    def step(index, carry):
        cols = pl.ds(pl.multiple_of(index * LANES, LANES), LANES)
        for k, out in enumerate(outs):
            rows = slice(k * slots, (k + 1) * slots)
            total = ins[0][rows, cols].astype(jnp.float32)
            for ref in ins[1:]:
                total = total + ref[rows, cols].astype(jnp.float32)
            out[:, cols] = total.astype(jnp.bfloat16)
        return carry

    lax.fori_loop(0, SPLIT // LANES, step, 0)
    for k, out in enumerate(outs):
        add_narrow(ins, slice(k * slots, (k + 1) * slots), out)


def sum_b_kernel(slots, place, *refs):
    ins, out = refs[:-1], refs[-1]
    peers, owners, capacity = out.shape[0], out.shape[1], out.shape[2]

    def step(k, carry):
        rows = pl.ds(pl.multiple_of(k * slots, slots), slots)
        target = lax.rem(place[0] + k, peers)
        total = ins[0][rows, :].astype(jnp.float32)
        for ref in ins[1:]:
            total = total + ref[rows, :].astype(jnp.float32)
        total = total.astype(jnp.bfloat16)
        for e in range(owners):
            out[target, e] = total[e * capacity : (e + 1) * capacity]
        return carry

    lax.fori_loop(0, peers, step, 0)


def last_kernel(*refs):
    ins, out = refs[:-1], refs[-1]

    def step(index, carry):
        cols = pl.ds(pl.multiple_of(index * STEP, STEP), STEP)
        total = ins[0][:, cols].astype(jnp.float32)
        for ref in ins[1:]:
            total = total + ref[:, cols].astype(jnp.float32)
        out[:, cols] = total.astype(jnp.bfloat16)
        return carry

    lax.fori_loop(0, SPLIT // STEP, step, 0)
    add_narrow(ins, slice(None), out)


def cost(count):
    return pl.CostEstimate(flops=count, bytes_accessed=3 * count, transcendentals=0)


def on_device(tokens, out_grad, expert_ids, gates, w_gate, w_up, w_down):
    token_count = tokens.shape[0]
    fan_out = expert_ids.shape[1]
    model_width = tokens.shape[1]
    owners = lax.axis_size("expert")
    rows_y = lax.axis_size(Y)
    rows_z = lax.axis_size(Z)
    capacity = max(2, 4 * token_count * fan_out // (3 * owners))
    slots = owners * capacity
    bf = jnp.bfloat16
    flat_ids = expert_ids.reshape(-1)
    sequence_pos = jnp.arange(token_count * fan_out, dtype=jnp.int32)
    earlier = sequence_pos[None, :] < sequence_pos[:, None]
    same_expert = flat_ids[:, None] == flat_ids[None, :]
    slot_rank = jnp.sum(jnp.logical_and(same_expert, earlier), axis=1)
    target = flat_ids * capacity + slot_rank
    token_hot = (target[:, None] == jnp.arange(slots, dtype=jnp.int32)[None, :]).astype(jnp.float32)
    token_hot = token_hot.reshape(token_count, fan_out, slots)
    dispatch = jnp.sum(token_hot, axis=1).astype(bf)
    slot_gate = jnp.sum(token_hot * gates[:, :, None], axis=(0, 1))
    send_tokens = lax.dot_general(dispatch, tokens, LEADING, preferred_element_type=jnp.float32)
    send_scaled = slot_gate[:, None] * lax.dot_general(
        dispatch, out_grad, LEADING, preferred_element_type=jnp.float32
    )
    owned = lax.all_to_all(
        send_tokens.astype(bf).reshape(owners, capacity, model_width),
        "expert",
        0,
        0,
        tiled=True,
    ).reshape(slots, model_width)
    copies = jnp.broadcast_to(
        send_scaled.astype(bf).reshape(1, owners, capacity, model_width),
        (rows_y, owners, capacity, model_width),
    ).reshape(rows_y * owners, capacity, model_width)
    copies, place = lax.optimization_barrier((copies, lax.axis_index(Y).reshape(1)))
    scaled_y = lax.all_to_all(copies, (Y, "expert"), 0, 0, tiled=True).reshape(
        rows_y * slots, model_width
    )
    tokens_z = jnp.concatenate(ring(owned, Z, split=False), axis=0)
    touch_call([w_gate[0], w_up[0], w_down[0]])
    token_blocks = ring(tokens_z, Y)
    scaled_blocks = ring(scaled_y, Z)
    (gathered, scaled, hidden, gate_pre_grad, up_pre_grad), out_a, out_b = main_call(
        place, token_blocks, scaled_blocks, w_gate[0], w_up[0], w_down[0], rows_y, rows_z, slots
    )
    arrived_b = [pass_on(out_b[k], Z, -k) for k in far_first(rows_z)]
    arrived_a = [pass_on(out_a[k], Y, -k) for k in range(1, rows_y)]
    grad_down = lax.dot_general(
        hidden, scaled, LEADING, preferred_element_type=jnp.float32
    ).astype(bf)
    grad_gate = lax.dot_general(
        gate_pre_grad, gathered, LEADING, preferred_element_type=jnp.float32
    ).astype(bf)
    grad_up = lax.dot_general(
        up_pre_grad, gathered, LEADING, preferred_element_type=jnp.float32
    ).astype(bf)
    wide = SPLIT + LANES
    narrow = model_width - SPLIT
    tiles_b = pl.pallas_call(
        functools.partial(sum_b_kernel, slots),
        out_shape=jax.ShapeDtypeStruct((rows_y, owners, capacity, narrow), bf),
        in_specs=[SMEM] + [VMEM] * rows_z,
        out_specs=VMEM,
        compiler_params=SMALL,
        cost_estimate=cost(rows_y * rows_z * slots * narrow),
        name="sum_z",
    )(place, out_b[0], *arrived_b)
    back_b = lax.all_to_all(
        tiles_b.reshape(rows_y * owners, capacity, narrow), (Y, "expert"), 0, 0, tiled=True
    ).reshape(rows_y * slots, narrow)
    tiles_a = pl.pallas_call(
        functools.partial(sum_a_kernel, slots),
        out_shape=[jax.ShapeDtypeStruct((slots, wide), bf)] * rows_z,
        in_specs=[VMEM] * rows_y,
        out_specs=[VMEM] * rows_z,
        compiler_params=SMALL,
        cost_estimate=cost(rows_y * rows_z * slots * wide),
        name="sum_y",
    )(out_a[0], *arrived_a)
    moved_a = [pass_on(tiles_a[k], Z, -k) for k in far_first(rows_z)]
    slot_home = pl.pallas_call(
        last_kernel,
        out_shape=jax.ShapeDtypeStruct((slots, wide), bf),
        in_specs=[VMEM] * rows_z,
        out_specs=VMEM,
        compiler_params=SMALL,
        cost_estimate=cost(rows_z * slots * wide),
        name="sum_home",
    )(tiles_a[0], *moved_a)
    back_a = lax.all_to_all(
        slot_home.reshape(owners, capacity, wide), "expert", 0, 0, tiled=True
    ).reshape(slots, wide)

    def combine(times, value):
        return jnp.dot(
            jnp.concatenate([dispatch] * times, axis=1), value, preferred_element_type=jnp.float32
        )

    input_grad = jnp.concatenate(
        [combine(1, back_a[:, :SPLIT]), combine(rows_y, back_b)], axis=1
    ).astype(bf)
    returned = joined(back_a[:, SPLIT:])
    product = jnp.sum(token_hot * returned[None, None, :, 0], axis=2)
    gate_grad = product / gates
    return (gate_grad, input_grad, grad_gate[None], grad_up[None], grad_down[None])


def solution(mesh):
    torus = Mesh(
        mesh.devices.reshape(mesh.shape["expert"], 4, 8), ("expert", "replica_0", "replica_1")
    )
    in_specs = (
        P(EXPERT_REPLICA, None),
        P(EXPERT_REPLICA, None),
        P(EXPERT_REPLICA, None),
        P(EXPERT_REPLICA, None),
        P("expert", REPLICA, None),
        P("expert", REPLICA, None),
        P("expert", REPLICA, None),
    )
    out_specs = (
        P(EXPERT_REPLICA, None),
        P(EXPERT_REPLICA, None),
        P("expert", REPLICA, None),
        P("expert", REPLICA, None),
        P("expert", REPLICA, None),
    )

    return jax.shard_map(
        on_device, mesh=torus, in_specs=in_specs, out_specs=out_specs, check_vma=False
    )
```
